32 devices in a mesh: ctx: 4 (over z), head: 4 (over y, x), grp: 2 (over core).
Axes of the slice: x: 2, y: 2, z: 4, core: 2. Of those that a mesh axis runs over, the one named last changes fastest.
Arguments:
- prompt_queries: bfloat16 [4096, 8192], P(('ctx', 'grp'), 'head'), may hold values from -16 to 16
- rotated_prompt_keys: bfloat16 [4096, 1024], P(('ctx', 'grp'), 'head'), may hold values from -12 to 12
- prompt_value_rows: bfloat16 [4096, 1024], P(('ctx', 'grp'), 'head'), may hold values from -12 to 12
- continuation_queries: bfloat16 [384, 8192], P(('ctx', 'grp'), 'head'), may hold values from -16 to 16
- prefix_len: int32 [384], replicated, may hold values from 2 to 4096
- out_weight: bfloat16 [8192, 8192], P('head', ('ctx', 'grp')), may hold values from -0.0625 to 0.0625
Outputs:
- prompt_context: bfloat16 [4096, 8192], P(('ctx', 'grp'), 'head')
- mixed: bfloat16 [384, 8192], P('head', ('ctx', 'grp'))
The draws below stay inside these ranges and needn't reach their ends.
Inputs may be any that keep to these rules, and one draw needn't show every extreme that they name: Continuation b reads prompt positions 0 to prefix_len[b] - 1.
All inputs are finite; a program needn't handle non-finite values.
Results may differ from the reference program's by a relative error of at most 0.018.
Values may be sent and summed in bfloat16 or wider, within the bound.
No kernel may reach another device: no remote copies, remote signals or barrier semaphores. Data moves between devices by JAX's collectives and lax.ppermute only.
A program may use at most 128 MiB of HBM per device.

```python
import jax
import jax.numpy as jnp
from jax import lax

D = 8192
QUERY_HEADS = 64
KEY_VALUE_HEADS = 8
HEAD_WIDTH = 128
PROMPT_LENGTH = 4096
CONTINUATION_NUM = 384


def drawn_queries(key, salt, total_rows, heads):
    random_jitter = jnp.clip(1.6 * jax.random.normal(jax.random.fold_in(key, salt), (total_rows, heads, HEAD_WIDTH), jnp.float32), -8.0, 8.0)
    return random_jitter.reshape(total_rows, heads * HEAD_WIDTH).astype(jnp.bfloat16)


def draw_prompt_queries(key, part):
    return drawn_queries(key, 11, PROMPT_LENGTH, QUERY_HEADS)


def draw_continuation_queries(key, part):
    return drawn_queries(key, 13, CONTINUATION_NUM, QUERY_HEADS)


def draw_rotated_prompt_keys(key, part):
    random_jitter = jnp.clip(1.6 * jax.random.normal(jax.random.fold_in(key, 12), (PROMPT_LENGTH, KEY_VALUE_HEADS, HEAD_WIDTH), jnp.float32), -8.0, 8.0)
    return random_jitter.reshape(PROMPT_LENGTH, KEY_VALUE_HEADS * HEAD_WIDTH).astype(jnp.bfloat16)


def plant(entries, rng, least, high):
    index_at = [jax.random.randint(jax.random.fold_in(rng, axis), (), 0, length) for axis, length in enumerate(entries.shape)]
    longest = entries.shape.index(max(entries.shape))
    beside = index_at[:longest] + [(index_at[longest] + 1) % entries.shape[longest]] + index_at[longest + 1:]
    return entries.at[tuple(index_at)].set(least).at[tuple(beside)].set(high)


def block_scale(key, extent, shards, low, high):
    def one(axis_at, parts):
        heights = jax.random.uniform(jax.random.fold_in(jax.random.fold_in(key, 6), axis_at), (parts,), jnp.float32, low / len(shards), high / len(shards))
        return jnp.repeat(jnp.exp(heights), extent[axis_at] // parts).reshape((-1,) + (1,) * (len(extent) - axis_at - 1))

    loudness = one(*shards[0])
    for cut in shards[1:]:
        loudness = loudness * one(*cut)
    return loudness


def bell_draw(rng, extent, deviation, limit, pieces=(), kind=jnp.bfloat16):
    entries = deviation * jax.random.normal(rng, extent, jnp.float32)
    if pieces:
        entries = entries * block_scale(rng, extent, pieces, -0.22, 0.18)
    return jnp.clip(entries, -limit, limit).astype(kind)


def setup_inputs(seed: int = 0) -> dict:
    seeds = jax.random.split(jax.random.key(seed), 7)
    prompt_queries = draw_prompt_queries(jax.random.fold_in(seeds[6], 71), 0)
    rotated_prompt_keys = draw_rotated_prompt_keys(jax.random.fold_in(seeds[6], 71), 0)
    prompt_value_rows = bell_draw(seeds[2], (PROMPT_LENGTH, KEY_VALUE_HEADS * HEAD_WIDTH), 2.0, 12.0, ((0, 8), (1, 4)))
    continuation_queries = draw_continuation_queries(jax.random.fold_in(seeds[6], 71), 0)
    prefix_len = plant(jax.random.randint(seeds[4], (CONTINUATION_NUM,), 2, PROMPT_LENGTH + 1), jax.random.fold_in(seeds[4], 1), 2, PROMPT_LENGTH).astype(jnp.int32)
    out_weight = bell_draw(seeds[5], (QUERY_HEADS * HEAD_WIDTH, D), (QUERY_HEADS * HEAD_WIDTH) ** -0.5, 0.0625, ((0, 4), (1, 8)))
    return dict(prompt_queries=prompt_queries, rotated_prompt_keys=rotated_prompt_keys, prompt_value_rows=prompt_value_rows, continuation_queries=continuation_queries, prefix_len=prefix_len, out_weight=out_weight)


NEG = -1e30


def softmax_rows(queries, key_rows, value_rows, allowed):
    scores = jnp.dot(queries.astype(jnp.float32), key_rows.astype(jnp.float32).T) * (HEAD_WIDTH ** -0.5)
    scores = jnp.where(allowed, scores, NEG)
    highest = jnp.max(scores, axis=1, keepdims=True)
    powers = jnp.exp(scores - highest)
    totals = jnp.sum(powers, axis=1, keepdims=True)
    rounded = lax.optimization_barrier(powers.astype(jnp.bfloat16))
    weighted = jnp.dot(rounded.astype(jnp.float32), value_rows.astype(jnp.float32))
    return (weighted / totals).astype(jnp.bfloat16)


def reference(prompt_queries, rotated_prompt_keys, prompt_value_rows, continuation_queries, prefix_len, out_weight):
    query_group_count = QUERY_HEADS // KEY_VALUE_HEADS
    places = jnp.arange(PROMPT_LENGTH, dtype=jnp.int32)
    expanded_key_heads = rotated_prompt_keys.reshape(PROMPT_LENGTH, KEY_VALUE_HEADS, HEAD_WIDTH).transpose(1, 0, 2)
    expanded_value_heads = prompt_value_rows.reshape(PROMPT_LENGTH, KEY_VALUE_HEADS, HEAD_WIDTH).transpose(1, 0, 2)

    def prompt_head(triple):
        queries, key_rows, value_rows = triple
        allowed = places[None, :] <= places[:, None]
        return softmax_rows(queries, key_rows, value_rows, allowed)

    query_heads = prompt_queries.reshape(PROMPT_LENGTH, QUERY_HEADS, HEAD_WIDTH).transpose(1, 0, 2)
    prompt_out = lax.map(prompt_head, (query_heads, jnp.repeat(expanded_key_heads, query_group_count, axis=0), jnp.repeat(expanded_value_heads, query_group_count, axis=0)))
    prompt_context = prompt_out.transpose(1, 0, 2).reshape(PROMPT_LENGTH, QUERY_HEADS * HEAD_WIDTH)

    lengths_rows = jnp.repeat(prefix_len, query_group_count)

    def decode_head(triple):
        queries, key_rows, value_rows = triple
        allowed = places[None, :] < lengths_rows[:, None]
        return softmax_rows(queries, key_rows, value_rows, allowed)

    continuation_rows = continuation_queries.reshape(CONTINUATION_NUM, KEY_VALUE_HEADS, query_group_count, HEAD_WIDTH).transpose(1, 0, 2, 3).reshape(KEY_VALUE_HEADS, CONTINUATION_NUM * query_group_count, HEAD_WIDTH)
    continuation_output = lax.map(decode_head, (continuation_rows, expanded_key_heads, expanded_value_heads))
    continuation_context = continuation_output.reshape(KEY_VALUE_HEADS, CONTINUATION_NUM, query_group_count, HEAD_WIDTH).transpose(1, 0, 2, 3).reshape(CONTINUATION_NUM, QUERY_HEADS * HEAD_WIDTH)
    mixed = jnp.dot(continuation_context.astype(jnp.float32), out_weight.astype(jnp.float32)).astype(jnp.bfloat16)
    return (prompt_context, mixed)
```

```python
import functools
import math

import jax
import jax.numpy as jnp
from jax import lax
from jax.experimental import pallas as pl
from jax.experimental.pallas import tpu as pltpu
from jax.sharding import PartitionSpec as P

QUERY_HEADS = 64
KEY_VALUE_HEADS = 8
HEAD_WIDTH = 128
GROUP = QUERY_HEADS // KEY_VALUE_HEADS

NEG = -1e30
SCALE = HEAD_WIDTH ** -0.5 * math.log2(math.e)
VMEM_BYTES = 60 * 1024 * 1024


def split_scaled(rows):
    scaled = rows.astype(jnp.float32) * SCALE
    high = scaled.astype(jnp.bfloat16)
    low = (scaled - high.astype(jnp.float32)).astype(jnp.bfloat16)
    return high, low


def score_tile(keys, queries):
    return lax.dot_general(
        jnp.concatenate([keys, keys], axis=1),
        queries,
        (((1,), (1,)), ((), ())),
        preferred_element_type=jnp.float32,
    )


def fold_tile(scores, values, acc_ref, unit, maxima, totals):
    raised = jnp.maximum(maxima, jnp.max(scores, axis=0, keepdims=True))
    powers = jnp.exp2(scores - raised)
    factor = jnp.exp2(maxima - raised)
    totals = totals * factor + jnp.sum(powers, axis=0, keepdims=True)
    acc_ref[unit] = acc_ref[unit] * factor + jnp.dot(
        values, powers.astype(jnp.bfloat16), preferred_element_type=jnp.float32
    )
    return raised, totals


def fold_units(score_of, values_of, acc_ref, state):
    result = []
    scores = score_of(0)
    for unit, (maxima, totals) in enumerate(state):
        following = score_of(unit + 1) if unit + 1 < len(state) else None
        result.append(fold_tile(scores, values_of(unit), acc_ref, unit, maxima, totals))
        scores = following
    return tuple(result)


def fresh(units, width):
    return tuple(
        (jnp.full((1, width), NEG, jnp.float32), jnp.zeros((1, width), jnp.float32))
        for _ in range(units)
    )


def prompt_kernel(index_ref, q_ref, k_ref, v_ref, o_ref, acc_ref, split_ref):
    rows = q_ref.shape[0]
    units = split_ref.shape[0]
    width = HEAD_WIDTH
    last = index_ref[0]
    acc_ref[...] = jnp.zeros_like(acc_ref)
    for unit in range(units):
        high, low = split_scaled(q_ref[:, unit * width : (unit + 1) * width])
        split_ref[unit, :, :width] = high
        split_ref[unit, :, width:] = low

    def block(number, state, diagonal):
        keys = k_ref[pl.ds(pl.multiple_of(number * rows, rows), rows), :]
        values = v_ref[number]

        def score_of(unit):
            scores = score_tile(keys, split_ref[unit])
            if diagonal:
                key_at = lax.broadcasted_iota(jnp.int32, scores.shape, 0)
                row_at = lax.broadcasted_iota(jnp.int32, scores.shape, 1)
                scores = jnp.where(key_at <= row_at, scores, NEG)
            return scores

        return fold_units(score_of, lambda unit: values, acc_ref, state)

    state = lax.fori_loop(
        0, last, lambda number, s: block(number, s, False), fresh(units, rows)
    )
    state = block(last, state, True)
    for unit in range(units):
        o_ref[:, unit * width : (unit + 1) * width] = (
            (acc_ref[unit] / state[unit][1]).T.astype(o_ref.dtype)
        )


def prompt_attention(my_index, queries, keys, values):
    rows, columns = queries.shape
    units = GROUP
    blocks = values.shape[0]
    scores = rows * keys.shape[0] * columns // HEAD_WIDTH
    return pl.pallas_call(
        prompt_kernel,
        out_shape=jax.ShapeDtypeStruct(queries.shape, queries.dtype),
        grid_spec=pltpu.PrefetchScalarGridSpec(
            num_scalar_prefetch=1,
            grid=(columns // (units * HEAD_WIDTH),),
            in_specs=[
                pl.BlockSpec((rows, units * HEAD_WIDTH), lambda g, i: (0, g)),
                pl.BlockSpec((keys.shape[0], HEAD_WIDTH), lambda g, i: (0, g)),
                pl.BlockSpec((blocks, HEAD_WIDTH, rows), lambda g, i: (0, g, 0)),
            ],
            out_specs=pl.BlockSpec((rows, units * HEAD_WIDTH), lambda g, i: (0, g)),
            scratch_shapes=[
                pltpu.VMEM((units, HEAD_WIDTH, rows), jnp.float32),
                pltpu.VMEM((units, rows, 2 * HEAD_WIDTH), jnp.bfloat16),
            ],
        ),
        compiler_params=pltpu.CompilerParams(vmem_limit_bytes=VMEM_BYTES),
        cost_estimate=pl.CostEstimate(
            flops=4 * scores * HEAD_WIDTH, bytes_accessed=8 * queries.size, transcendentals=scores
        ),
    )(my_index, queries, keys, values)


def decode_kernel(q_ref, k_ref, v_ref, len_ref, o_ref, acc_ref, split_ref):
    rows = q_ref.shape[0]
    units = split_ref.shape[0]
    blocks, _, block_rows = v_ref.shape
    width = HEAD_WIDTH
    acc_ref[...] = jnp.zeros_like(acc_ref)
    for unit in range(units):
        for member in range(GROUP):
            head = unit * GROUP + member
            high, low = split_scaled(q_ref[:, head * width : (head + 1) * width])
            split_ref[unit, member * rows : (member + 1) * rows, :width] = high
            split_ref[unit, member * rows : (member + 1) * rows, width:] = low
    lengths = len_ref[...]

    def block(number, state):
        first = pl.multiple_of(number * block_rows, block_rows)

        def score_of(unit):
            keys = k_ref[pl.ds(first, block_rows), unit * width : (unit + 1) * width]
            scores = score_tile(keys, split_ref[unit])
            key_at = lax.broadcasted_iota(jnp.int32, scores.shape, 0)
            return jnp.where(key_at < lengths - first, scores, NEG)

        def values_of(unit):
            return v_ref[number, unit * width : (unit + 1) * width, :]

        return fold_units(score_of, values_of, acc_ref, state)

    state = lax.fori_loop(0, blocks, block, fresh(units, rows * GROUP))
    for unit in range(units):
        context = (acc_ref[unit] / state[unit][1]).T.astype(o_ref.dtype)
        for member in range(GROUP):
            head = unit * GROUP + member
            o_ref[:, head * width : (head + 1) * width] = context[
                member * rows : (member + 1) * rows
            ]


def decode_attention(queries, keys, values, lengths):
    rows, columns = queries.shape
    units = columns // (GROUP * HEAD_WIDTH)
    lanes = jnp.tile(lengths, GROUP)[None, :]
    scores = rows * keys.shape[0] * columns // HEAD_WIDTH
    return pl.pallas_call(
        decode_kernel,
        out_shape=jax.ShapeDtypeStruct(queries.shape, queries.dtype),
        scratch_shapes=[
            pltpu.VMEM((units, HEAD_WIDTH, rows * GROUP), jnp.float32),
            pltpu.VMEM((units, rows * GROUP, 2 * HEAD_WIDTH), jnp.bfloat16),
        ],
        compiler_params=pltpu.CompilerParams(vmem_limit_bytes=VMEM_BYTES),
        cost_estimate=pl.CostEstimate(
            flops=4 * scores * HEAD_WIDTH, bytes_accessed=4 * keys.size, transcendentals=scores
        ),
    )(queries, keys, values, lanes)


def local(
    prompt_queries,
    rotated_prompt_keys,
    prompt_value_rows,
    continuation_queries,
    prefix_len,
    out_weight,
):
    along = ("ctx", "grp")
    my_index = lax.axis_index(along)
    keys = lax.all_gather(rotated_prompt_keys, along, axis=0, tiled=True)
    values = lax.all_gather(prompt_value_rows.T, along, axis=0)

    own_rows = continuation_queries.shape[0]
    lengths = lax.dynamic_slice_in_dim(prefix_len, my_index * own_rows, own_rows, 0)
    continuation_context = decode_attention(continuation_queries, keys, values, lengths)
    gathered = lax.all_gather(continuation_context, along, axis=0, tiled=True)
    mixed = lax.psum_scatter(
        jnp.dot(gathered, out_weight, preferred_element_type=jnp.float32).astype(jnp.bfloat16),
        "head",
        scatter_dimension=0,
        tiled=True,
    )
    prompt_context = prompt_attention(my_index[None].astype(jnp.int32), prompt_queries, keys, values)
    return (prompt_context, mixed)


def solution(mesh):
    in_specs = (
        P(("ctx", "grp"), "head"),
        P(("ctx", "grp"), "head"),
        P(("ctx", "grp"), "head"),
        P(("ctx", "grp"), "head"),
        P(),
        P("head", ("ctx", "grp")),
    )
    out_specs = (P(("ctx", "grp"), "head"), P("head", ("ctx", "grp")))
    return jax.shard_map(local, mesh=mesh, in_specs=in_specs, out_specs=out_specs, check_vma=False)
```

```python
import functools
import math

import jax
import jax.numpy as jnp
from jax import lax
from jax.experimental import pallas as pl
from jax.experimental.pallas import tpu as pltpu
from jax.sharding import PartitionSpec as P

QUERY_HEADS = 64
KEY_VALUE_HEADS = 8
HEAD_WIDTH = 128
GROUP = QUERY_HEADS // KEY_VALUE_HEADS
UNITS = GROUP // 2

NEG = -1e30
SCALE = HEAD_WIDTH ** -0.5 * math.log2(math.e)
BOUND = 2.0**64
MIB = 1024 * 1024


def split_scaled(rows):
    scaled = rows.astype(jnp.float32) * SCALE
    high = scaled.astype(jnp.bfloat16)
    low = (scaled - high.astype(jnp.float32)).astype(jnp.bfloat16)
    return high, low


def score_tile(keys, queries):
    return lax.dot_general(
        jnp.concatenate([keys, keys], axis=1),
        queries,
        (((1,), (1,)), ((), ())),
        preferred_element_type=jnp.float32,
    )


def row_sums(powers):
    return jnp.sum(powers.reshape(-1, 8, powers.shape[1]), axis=0)


def pipelined(items, first, second, third):
    ahead = first(items[0])
    behind = None
    for place, item in enumerate(items):
        following = first(items[place + 1]) if place + 1 < len(items) else None
        if behind is not None:
            third(items[place - 1], behind)
        behind = second(item, ahead)
        ahead = following
    third(items[-1], behind)


def fill_split(q_ref, split_ref):
    for unit in range(split_ref.shape[0]):
        columns = slice(unit * HEAD_WIDTH, (unit + 1) * HEAD_WIDTH)
        high, low = split_scaled(q_ref[:, columns])
        split_ref[unit, :, :HEAD_WIDTH] = high
        split_ref[unit, :, HEAD_WIDTH:] = low


def later_blocks(key_refs, value_refs, split_ref, old, new):
    acc_old, sum_old, max_old = old
    acc_new, sum_new, max_new = new
    units = split_ref.shape[0]
    values = [ref[...].T for ref in value_refs]
    max_new[...] = max_old[...]

    def score(item):
        block, unit = item
        return score_tile(key_refs[block][...], split_ref[unit])

    def power(item, scores):
        block, unit = item
        powers = jnp.exp2(scores - max_old[unit])
        earlier = (sum_old if block == 0 else sum_new)[unit]
        sum_new[unit] = earlier + row_sums(powers)
        return powers.astype(jnp.bfloat16)

    def weigh(item, powers):
        block, unit = item
        earlier = (acc_old if block == 0 else acc_new)[unit]
        acc_new[unit] = earlier + jnp.dot(
            values[block], powers, preferred_element_type=jnp.float32
        )

    pipelined(
        [(block, unit) for block in range(len(key_refs)) for unit in range(units)],
        score,
        power,
        weigh,
    )

    @pl.when(jnp.max(sum_new[...]) > BOUND)
    def _():
        def one(unit, carry):
            acc, total, top = acc_old[unit], sum_old[unit], max_old[unit]
            for key_ref, value in zip(key_refs, values):
                scores = score_tile(key_ref[...], split_ref[unit])
                raised = jnp.maximum(top, jnp.max(scores, axis=0, keepdims=True))
                powers = jnp.exp2(scores - raised)
                factor = jnp.exp2(top - raised)
                total = total * factor + row_sums(powers)
                acc = acc * factor + jnp.dot(
                    value, powers.astype(jnp.bfloat16), preferred_element_type=jnp.float32
                )
                top = raised
            acc_new[unit], sum_new[unit], max_new[unit] = acc, total, top
            return carry

        lax.fori_loop(0, units, one, 0)


def write_context(o_ref, acc_ref, sum_ref):
    for unit in range(acc_ref.shape[0]):
        total = jnp.sum(sum_ref[unit], axis=0, keepdims=True)
        o_ref[:, unit * HEAD_WIDTH : (unit + 1) * HEAD_WIDTH] = (
            (acc_ref[unit] / total).T.astype(o_ref.dtype)
        )


def first_stage_kernel(
    flag_ref, q_ref, k_ref, v_ref, ko_ref, vo_ref, acc_ref, sum_ref, max_ref,
    split_ref, acc_own, sum_own, max_own,
):
    fill_split(q_ref, split_ref)
    values = v_ref[...].T

    def score(unit):
        scores = score_tile(k_ref[...], split_ref[unit])
        key_at = lax.broadcasted_iota(jnp.int32, scores.shape, 0)
        row_at = lax.broadcasted_iota(jnp.int32, scores.shape, 1)
        return jnp.where(key_at <= row_at, scores, NEG)

    def power(unit, scores):
        top = jnp.max(scores, axis=0, keepdims=True)
        powers = jnp.exp2(scores - top)
        max_own[unit] = top
        sum_own[unit] = row_sums(powers)
        return powers.astype(jnp.bfloat16)

    def weigh(unit, powers):
        acc_own[unit] = jnp.dot(values, powers, preferred_element_type=jnp.float32)

    pipelined(list(range(split_ref.shape[0])), score, power, weigh)
    own, out = (acc_own, sum_own, max_own), (acc_ref, sum_ref, max_ref)

    @pl.when(flag_ref[0] == 0)
    def _():
        for source, target in zip(own, out):
            target[...] = source[...]

    @pl.when(flag_ref[0] != 0)
    def _():
        later_blocks([ko_ref], [vo_ref], split_ref, own, out)


def middle_stage_kernel(
    flag_ref, q_ref, k_ref, v_ref, ko_ref, vo_ref, acc_in, sum_in, max_in,
    acc_ref, sum_ref, max_ref, split_ref,
):
    old, new = (acc_in, sum_in, max_in), (acc_ref, sum_ref, max_ref)

    @pl.when(flag_ref[0] == 0)
    def _():
        for source, target in zip(old, new):
            target[...] = source[...]

    @pl.when(flag_ref[0] != 0)
    def _():
        fill_split(q_ref, split_ref)
        later_blocks([k_ref, ko_ref], [v_ref, vo_ref], split_ref, old, new)


def last_stage_kernel(
    flag_ref, q_ref, k_ref, v_ref, ko_ref, vo_ref, acc_in, sum_in, max_in, o_ref,
    split_ref, acc_ref, sum_ref, max_ref,
):
    @pl.when(flag_ref[0] == 0)
    def _():
        write_context(o_ref, acc_in, sum_in)

    @pl.when(flag_ref[0] != 0)
    def _():
        fill_split(q_ref, split_ref)
        later_blocks(
            [k_ref, ko_ref],
            [v_ref, vo_ref],
            split_ref,
            (acc_in, sum_in, max_in),
            (acc_ref, sum_ref, max_ref),
        )
        write_context(o_ref, acc_ref, sum_ref)


def prompt_stage(kind, flag, queries, mine, other, state=()):
    rows, columns = queries.shape
    heads = columns // HEAD_WIDTH
    heads_kv = mine.shape[1] // (2 * HEAD_WIDTH)
    steps_each = GROUP // UNITS
    wide = pl.BlockSpec((rows, UNITS * HEAD_WIDTH), lambda h, f: (0, h))
    key_spec = pl.BlockSpec((rows, HEAD_WIDTH), lambda h, f: (0, h // steps_each))
    value_spec = pl.BlockSpec((rows, HEAD_WIDTH), lambda h, f: (0, heads_kv + h // steps_each))
    depths = (HEAD_WIDTH, 8, 1)
    state_specs = [pl.BlockSpec((UNITS, depth, rows), lambda h, f: (h, 0, 0)) for depth in depths]
    state_shapes = [jax.ShapeDtypeStruct((heads, depth, rows), jnp.float32) for depth in depths]
    scratch = [pltpu.VMEM((UNITS, rows, 2 * HEAD_WIDTH), jnp.bfloat16)]
    own_state = [pltpu.VMEM((UNITS, depth, rows), jnp.float32) for depth in depths]
    if kind == "first":
        body, out_shape, out_specs = first_stage_kernel, state_shapes, state_specs
        scratch += own_state
    elif kind == "middle":
        body, out_shape, out_specs = middle_stage_kernel, state_shapes, state_specs
    else:
        body, out_specs = last_stage_kernel, wide
        out_shape = jax.ShapeDtypeStruct(queries.shape, queries.dtype)
        scratch += own_state
    scores = 2 * rows * rows * heads
    return pl.pallas_call(
        body,
        out_shape=out_shape,
        grid_spec=pltpu.PrefetchScalarGridSpec(
            num_scalar_prefetch=1,
            grid=(heads // UNITS,),
            in_specs=[wide, key_spec, value_spec, key_spec, value_spec]
            + (state_specs if state else []),
            out_specs=out_specs,
            scratch_shapes=scratch,
        ),
        compiler_params=pltpu.CompilerParams(vmem_limit_bytes=60 * MIB),
        cost_estimate=pl.CostEstimate(
            flops=4 * scores * HEAD_WIDTH, bytes_accessed=8 * queries.size, transcendentals=scores
        ),
        name="prompt_" + kind,
    )(flag, queries, mine, mine, other, other, *state)


def decode_kernel(hops, place_ref, q_ref, len_ref, *refs):
    slots = 2 * (2 * hops + 1)
    pairs = refs[:slots]
    o_ref, kv_ref, split_ref, score_ref, acc_ref, sem = refs[slots:]
    rows = q_ref.shape[0]
    units = split_ref.shape[0]
    blocks, block_rows = kv_ref.shape[:2]
    width = HEAD_WIDTH
    chip, core = place_ref[0], place_ref[1]

    def each_copy(action):
        for slot in range(slots):
            at = chip + slot // 2 - hops
            block = 2 * at + (core if slot % 2 == 0 else 1 - core)

            @pl.when((at >= 0) & (at < blocks // 2))
            def _():
                action(pltpu.make_async_copy(pairs[slot], kv_ref.at[block], sem.at[slot]))

    each_copy(lambda copy: copy.start())
    for unit in range(units):
        for member in range(GROUP):
            head = unit * GROUP + member
            high, low = split_scaled(q_ref[:, head * width : (head + 1) * width])
            split_ref[unit, member * rows : (member + 1) * rows, :width] = high
            split_ref[unit, member * rows : (member + 1) * rows, width:] = low
    each_copy(lambda copy: copy.wait())
    lengths = len_ref[...]
    tops = [jnp.full((1, rows * GROUP), NEG, jnp.float32) for _ in range(units)]
    for block in range(blocks):
        for unit in range(units):
            keys = kv_ref[block, :, unit * width : (unit + 1) * width]
            scores = score_tile(keys, split_ref[unit])
            key_at = lax.broadcasted_iota(jnp.int32, scores.shape, 0)
            scores = jnp.where(key_at < lengths - block * block_rows, scores, NEG)
            score_ref[block, unit] = scores
            tops[unit] = jnp.maximum(tops[unit], jnp.max(scores, axis=0, keepdims=True))
    sums = [jnp.zeros((8, rows * GROUP), jnp.float32) for _ in range(units)]
    acc_ref[...] = jnp.zeros_like(acc_ref)

    def first(item):
        block, unit = item
        powers = jnp.exp2(score_ref[block, unit] - tops[unit])
        sums[unit] = sums[unit] + row_sums(powers)
        return powers.astype(jnp.bfloat16)

    def third(item, powers):
        block, unit = item
        values = kv_ref[block, :, (units + unit) * width : (units + unit + 1) * width].T
        acc_ref[unit] += jnp.dot(values, powers, preferred_element_type=jnp.float32)

    items = [(block, unit) for block in range(blocks) for unit in range(units)]
    pipelined(items, first, lambda item, powers: powers, third)
    for unit in range(units):
        total = jnp.sum(sums[unit], axis=0, keepdims=True)
        context = (acc_ref[unit] / total).T.astype(o_ref.dtype)
        for member in range(GROUP):
            head = unit * GROUP + member
            o_ref[:, head * width : (head + 1) * width] = context[
                member * rows : (member + 1) * rows
            ]


def decode_attention(place, queries, lengths, pairs, hops):
    rows, columns = queries.shape
    units = columns // (GROUP * HEAD_WIDTH)
    block_rows, block_columns = pairs[0].shape
    blocks = 2 * (hops + 1)
    lanes = jnp.tile(lengths, GROUP)[None, :]
    scores = rows * blocks * block_rows * columns // HEAD_WIDTH
    vmem = pl.BlockSpec(memory_space=pltpu.VMEM)
    return pl.pallas_call(
        functools.partial(decode_kernel, hops),
        out_shape=jax.ShapeDtypeStruct(queries.shape, queries.dtype),
        in_specs=[pl.BlockSpec(memory_space=pltpu.SMEM), vmem, vmem]
        + [pl.BlockSpec(memory_space=pl.ANY)] * len(pairs),
        out_specs=vmem,
        scratch_shapes=[
            pltpu.VMEM((blocks, block_rows, block_columns), jnp.bfloat16),
            pltpu.VMEM((units, rows * GROUP, 2 * HEAD_WIDTH), jnp.bfloat16),
            pltpu.VMEM((blocks, units, block_rows, rows * GROUP), jnp.float32),
            pltpu.VMEM((units, HEAD_WIDTH, rows * GROUP), jnp.float32),
            pltpu.SemaphoreType.DMA((len(pairs),)),
        ],
        compiler_params=pltpu.CompilerParams(vmem_limit_bytes=60 * MIB),
        cost_estimate=pl.CostEstimate(
            flops=4 * scores * HEAD_WIDTH,
            bytes_accessed=2 * blocks * block_rows * block_columns,
            transcendentals=scores,
        ),
        name="decode",
    )(place, queries, lanes, *pairs)


def shift(array, distance):
    count = lax.axis_size("ctx")
    pairs = [(i, i + distance) for i in range(count) if 0 <= i + distance < count]
    return lax.ppermute(array, "ctx", pairs)


def swap(array):
    return lax.ppermute(array, "grp", [(0, 1), (1, 0)])


def reduce_over_heads(partial):
    count = lax.axis_size("head")
    me = lax.axis_index("head")
    rows = partial.shape[0] // count

    def piece(number):
        return lax.dynamic_slice_in_dim(partial, number * rows, rows, 0)

    power_of_two = count & (count - 1) == 0
    total = piece(me).astype(jnp.float32)
    for step in range(1, count):
        if power_of_two:
            target, pairs = me ^ step, [(i, i ^ step) for i in range(count)]
        else:
            target = (me + step) % count
            pairs = [(i, (i + step) % count) for i in range(count)]
        total += lax.ppermute(piece(target), "head", pairs).astype(jnp.float32)
    return total.astype(partial.dtype)


def local(
    prompt_queries,
    rotated_prompt_keys,
    prompt_value_rows,
    continuation_queries,
    prefix_len,
    out_weight,
):
    chips = lax.axis_size("ctx")
    hops = chips - 1
    chip, core = lax.axis_index("ctx"), lax.axis_index("grp")
    own = jnp.concatenate([rotated_prompt_keys, prompt_value_rows], axis=1)
    pairs = {0: (own, swap(own))}
    state = None
    up = down = own
    for hop in range(hops + 1):
        if hop < hops:
            up, down = shift(up, 1), shift(down, -1)
        mine, other = pairs[-hop]
        flag = core if hop == 0 else chip >= hop
        kind = "first" if hop == 0 else "last" if hop == hops else "middle"
        if kind != "last":
            state = prompt_stage(
                kind, flag.astype(jnp.int32)[None], prompt_queries, mine, other, state or ()
            )
            up, down, state = lax.optimization_barrier((up, down, state))
            pairs[-hop - 1] = (up, swap(up))
            pairs[hop + 1] = (down, swap(down))

    own_rows = continuation_queries.shape[0]
    my_index = chip * 2 + core
    lengths = lax.dynamic_slice_in_dim(prefix_len, my_index * own_rows, own_rows, 0)
    ordered = [array for slot in range(-hops, hops + 1) for array in pairs[slot]]
    context = decode_attention(
        jnp.stack([chip, core]).astype(jnp.int32), continuation_queries, lengths, ordered, hops
    )
    spread = [shift(context, -slot) if slot else context for slot in range(-hops, hops + 1)]
    prompt_context = prompt_stage(
        "last", (chip >= hops).astype(jnp.int32)[None], prompt_queries, *pairs[-hops], state
    )
    prompt_context, spread = lax.optimization_barrier((prompt_context, spread))
    same_core = lax.dynamic_slice_in_dim(jnp.stack(spread), hops - chip, chips, 0)
    other_core = swap(same_core)
    gathered = jnp.where(
        core == 0,
        jnp.stack([same_core, other_core], axis=1),
        jnp.stack([other_core, same_core], axis=1),
    ).reshape(chips * 2 * own_rows, -1)
    partial = jnp.dot(gathered, out_weight, preferred_element_type=jnp.float32)
    mixed = reduce_over_heads(partial.astype(jnp.bfloat16))
    return (prompt_context, mixed)


def solution(mesh):
    in_specs = (
        P(("ctx", "grp"), "head"),
        P(("ctx", "grp"), "head"),
        P(("ctx", "grp"), "head"),
        P(("ctx", "grp"), "head"),
        P(),
        P("head", ("ctx", "grp")),
    )
    out_specs = (P(("ctx", "grp"), "head"), P("head", ("ctx", "grp")))
    return jax.shard_map(local, mesh=mesh, in_specs=in_specs, out_specs=out_specs, check_vma=False)
```

```python
import functools
import math

import jax
import jax.numpy as jnp
from jax import lax
from jax.experimental import pallas as pl
from jax.experimental.pallas import tpu as pltpu
from jax.sharding import PartitionSpec as P

QUERY_HEADS = 64
KEY_VALUE_HEADS = 8
HEAD_WIDTH = 128
GROUP = QUERY_HEADS // KEY_VALUE_HEADS
UNITS = GROUP // 2

NEG = -1e30
SCALE = HEAD_WIDTH ** -0.5 * math.log2(math.e)
BOUND = 2.0**64
MIB = 1024 * 1024


def split_scaled(rows):
    scaled = rows.astype(jnp.float32) * SCALE
    high = scaled.astype(jnp.bfloat16)
    low = (scaled - high.astype(jnp.float32)).astype(jnp.bfloat16)
    return high, low


def score_tile(keys, queries):
    return lax.dot_general(
        jnp.concatenate([keys, keys], axis=1),
        queries,
        (((1,), (1,)), ((), ())),
        preferred_element_type=jnp.float32,
    )


def row_sums(powers):
    return jnp.sum(powers.reshape(-1, 8, powers.shape[1]), axis=0)


def pipelined(items, first, second, third):
    ahead = first(items[0])
    behind = None
    for place, item in enumerate(items):
        following = first(items[place + 1]) if place + 1 < len(items) else None
        if behind is not None:
            third(items[place - 1], behind)
        behind = second(item, ahead)
        ahead = following
    third(items[-1], behind)


def fill_split(q_ref, split_ref):
    for unit in range(split_ref.shape[0]):
        columns = slice(unit * HEAD_WIDTH, (unit + 1) * HEAD_WIDTH)
        high, low = split_scaled(q_ref[:, columns])
        split_ref[unit, :, :HEAD_WIDTH] = high
        split_ref[unit, :, HEAD_WIDTH:] = low


def later_blocks(key_refs, value_refs, split_ref, old, new):
    acc_old, sum_old, max_old = old
    acc_new, sum_new, max_new = new
    units = split_ref.shape[0]
    values = [ref[...].T for ref in value_refs]
    max_new[...] = max_old[...]

    def score(item):
        block, unit = item
        return score_tile(key_refs[block][...], split_ref[unit])

    def power(item, scores):
        block, unit = item
        powers = jnp.exp2(scores - max_old[unit])
        earlier = (sum_old if block == 0 else sum_new)[unit]
        sum_new[unit] = earlier + row_sums(powers)
        return powers.astype(jnp.bfloat16)

    def weigh(item, powers):
        block, unit = item
        earlier = (acc_old if block == 0 else acc_new)[unit]
        acc_new[unit] = earlier + jnp.dot(
            values[block], powers, preferred_element_type=jnp.float32
        )

    pipelined(
        [(block, unit) for block in range(len(key_refs)) for unit in range(units)],
        score,
        power,
        weigh,
    )

    @pl.when(jnp.max(sum_new[...]) > BOUND)
    def _():
        def one(unit, carry):
            acc, total, top = acc_old[unit], sum_old[unit], max_old[unit]
            for key_ref, value in zip(key_refs, values):
                scores = score_tile(key_ref[...], split_ref[unit])
                raised = jnp.maximum(top, jnp.max(scores, axis=0, keepdims=True))
                powers = jnp.exp2(scores - raised)
                factor = jnp.exp2(top - raised)
                total = total * factor + row_sums(powers)
                acc = acc * factor + jnp.dot(
                    value, powers.astype(jnp.bfloat16), preferred_element_type=jnp.float32
                )
                top = raised
            acc_new[unit], sum_new[unit], max_new[unit] = acc, total, top
            return carry

        lax.fori_loop(0, units, one, 0)


def write_context(o_ref, acc_ref, sum_ref):
    for unit in range(acc_ref.shape[0]):
        total = jnp.sum(sum_ref[unit], axis=0, keepdims=True)
        o_ref[:, unit * HEAD_WIDTH : (unit + 1) * HEAD_WIDTH] = (
            (acc_ref[unit] / total).T.astype(o_ref.dtype)
        )


def run_stages(flag_ref, groups, split_ref, states):
    for number, (key_refs, value_refs) in enumerate(groups):
        old, new = states[number], states[number + 1]

        @pl.when(flag_ref[number] == 0)
        def _():
            for source, target in zip(old, new):
                target[...] = source[...]

        @pl.when(flag_ref[number] != 0)
        def _():
            later_blocks(key_refs, value_refs, split_ref, old, new)


def begin_kernel(sizes, flag_ref, q_ref, k_ref, v_ref, *refs):
    groups, refs = take_groups(sizes, refs)
    result, split_ref, scratch = refs[:3], refs[3], refs[4:]
    states = [tuple(scratch[i : i + 3]) for i in range(0, len(scratch), 3)] + [tuple(result)]
    acc_own, sum_own, max_own = states[0]
    fill_split(q_ref, split_ref)
    values = v_ref[...].T

    def score(unit):
        scores = score_tile(k_ref[...], split_ref[unit])
        key_at = lax.broadcasted_iota(jnp.int32, scores.shape, 0)
        row_at = lax.broadcasted_iota(jnp.int32, scores.shape, 1)
        return jnp.where(key_at <= row_at, scores, NEG)

    def power(unit, scores):
        top = jnp.max(scores, axis=0, keepdims=True)
        powers = jnp.exp2(scores - top)
        max_own[unit] = top
        sum_own[unit] = row_sums(powers)
        return powers.astype(jnp.bfloat16)

    def weigh(unit, powers):
        acc_own[unit] = jnp.dot(values, powers, preferred_element_type=jnp.float32)

    pipelined(list(range(split_ref.shape[0])), score, power, weigh)
    run_stages(flag_ref, groups, split_ref, states)


def end_kernel(sizes, flag_ref, q_ref, acc_in, sum_in, max_in, *refs):
    groups, refs = take_groups(sizes, refs)
    o_ref, split_ref, scratch = refs[0], refs[1], refs[2:]
    states = [(acc_in, sum_in, max_in)]
    pair = [tuple(scratch[:3]), tuple(scratch[3:])]
    states += [pair[number % 2] for number in range(len(groups))]

    @pl.when(flag_ref[0] == 0)
    def _():
        write_context(o_ref, acc_in, sum_in)

    @pl.when(flag_ref[0] != 0)
    def _():
        fill_split(q_ref, split_ref)
        run_stages(flag_ref, groups, split_ref, states)
        write_context(o_ref, *states[-1][:2])


def take_groups(sizes, refs):
    groups, refs = [], list(refs)
    for size in sizes:
        groups.append((refs[0 : 2 * size : 2], refs[1 : 2 * size : 2]))
        refs = refs[2 * size :]
    return groups, refs


def prompt_part(flags, queries, own, groups, state):
    rows, columns = queries.shape
    heads = columns // HEAD_WIDTH
    heads_kv = groups[0][0].shape[1] // (2 * HEAD_WIDTH)
    steps_each = GROUP // UNITS
    wide = pl.BlockSpec((rows, UNITS * HEAD_WIDTH), lambda h, f: (0, h))
    key_spec = pl.BlockSpec((rows, HEAD_WIDTH), lambda h, f: (0, h // steps_each))
    value_spec = pl.BlockSpec((rows, HEAD_WIDTH), lambda h, f: (0, heads_kv + h // steps_each))
    depths = (HEAD_WIDTH, 8, 1)
    state_specs = [pl.BlockSpec((UNITS, depth, rows), lambda h, f: (h, 0, 0)) for depth in depths]
    held = [pltpu.VMEM((UNITS, depth, rows), jnp.float32) for depth in depths]
    split = [pltpu.VMEM((UNITS, rows, 2 * HEAD_WIDTH), jnp.bfloat16)]
    sizes = tuple(len(group) for group in groups)
    blocks = [array for group in groups for array in group]
    if state is None:
        body, out_specs = begin_kernel, state_specs
        out_shape = [jax.ShapeDtypeStruct((heads, depth, rows), jnp.float32) for depth in depths]
        operands, specs = [own, own], [key_spec, value_spec]
        scratch = split + held * len(groups)
    else:
        body, out_specs = end_kernel, wide
        out_shape = jax.ShapeDtypeStruct(queries.shape, queries.dtype)
        operands, specs = list(state), state_specs
        scratch = split + held * 2
    scores = (len(blocks) + (state is None)) * rows * rows * heads
    return pl.pallas_call(
        functools.partial(body, sizes),
        out_shape=out_shape,
        grid_spec=pltpu.PrefetchScalarGridSpec(
            num_scalar_prefetch=1,
            grid=(heads // UNITS,),
            in_specs=[wide] + specs + [key_spec, value_spec] * len(blocks),
            out_specs=out_specs,
            scratch_shapes=scratch,
        ),
        compiler_params=pltpu.CompilerParams(vmem_limit_bytes=60 * MIB),
        cost_estimate=pl.CostEstimate(
            flops=4 * scores * HEAD_WIDTH, bytes_accessed=8 * queries.size, transcendentals=scores
        ),
        name="prompt_begin" if state is None else "prompt_end",
    )(flags.astype(jnp.int32), queries, *operands, *[a for block in blocks for a in (block, block)])


def decode_kernel(place_ref, q_ref, len_ref, *refs):
    slots = len(refs) - 6
    pairs = refs[:slots]
    o_ref, kv_ref, split_ref, acc_ref, sum_ref, sem = refs[slots:]
    rows = q_ref.shape[0]
    units = split_ref.shape[0]
    blocks, block_rows = kv_ref.shape[:2]
    width = HEAD_WIDTH
    chip, core = place_ref[0], place_ref[1]
    copies = []
    for slot in range(slots):
        at = chip - slot // 2
        at = jnp.where(at < 0, at + slots // 2, at)
        block = 2 * at + (core if slot % 2 == 0 else 1 - core)
        copies.append(pltpu.make_async_copy(pairs[slot], kv_ref.at[block], sem.at[slot]))
    for copy in copies:
        copy.start()
    for unit in range(units):
        for member in range(GROUP):
            head = unit * GROUP + member
            high, low = split_scaled(q_ref[:, head * width : (head + 1) * width])
            split_ref[unit, member * rows : (member + 1) * rows, :width] = high
            split_ref[unit, member * rows : (member + 1) * rows, width:] = low
    for copy in copies:
        copy.wait()
    lengths = len_ref[...]

    def masked(block, unit):
        columns = pl.ds(pl.multiple_of(unit * width, width), width)
        scores = score_tile(kv_ref[block, :, columns], split_ref[unit])
        key_at = lax.broadcasted_iota(jnp.int32, scores.shape, 0)
        return jnp.where(key_at < lengths - block * block_rows, scores, NEG)

    def values_of(block, unit):
        columns = pl.ds(pl.multiple_of((units + unit) * width, width), width)
        return kv_ref[block, :, columns].T

    tops = [None] * units

    def first(item):
        block, unit = item
        return masked(block, unit), values_of(block, unit)

    def second(item, ahead):
        (block, unit), (scores, values) = item, ahead
        if block == 0:
            tops[unit] = jnp.max(scores, axis=0, keepdims=True)
        powers = jnp.exp2(scores - tops[unit])
        sums = row_sums(powers)
        sum_ref[unit] = sums if block == 0 else sum_ref[unit] + sums
        return powers.astype(jnp.bfloat16), values

    def third(item, behind):
        (block, unit), (powers, values) = item, behind
        added = jnp.dot(values, powers, preferred_element_type=jnp.float32)
        acc_ref[unit] = added if block == 0 else acc_ref[unit] + added

    items = [(block, unit) for block in range(blocks) for unit in range(units)]
    pipelined(items, first, second, third)

    @pl.when(jnp.max(sum_ref[...]) > BOUND)
    def _():
        def one(unit, carry):
            acc_ref[unit] = jnp.zeros(acc_ref.shape[1:], jnp.float32)
            sum_ref[unit] = jnp.zeros(sum_ref.shape[1:], jnp.float32)

            def visit(block, top):
                scores = masked(block, unit)
                raised = jnp.maximum(top, jnp.max(scores, axis=0, keepdims=True))
                powers = jnp.exp2(scores - raised)
                factor = jnp.exp2(top - raised)
                sum_ref[unit] = sum_ref[unit] * factor + row_sums(powers)
                acc_ref[unit] = acc_ref[unit] * factor + jnp.dot(
                    values_of(block, unit),
                    powers.astype(jnp.bfloat16),
                    preferred_element_type=jnp.float32,
                )
                return raised

            lax.fori_loop(0, blocks, visit, jnp.full(lengths.shape, NEG, jnp.float32))
            return carry

        lax.fori_loop(0, units, one, 0)

    for unit in range(units):
        total = jnp.sum(sum_ref[unit], axis=0, keepdims=True)
        context = (acc_ref[unit] / total).T.astype(o_ref.dtype)
        for member in range(GROUP):
            head = unit * GROUP + member
            o_ref[:, head * width : (head + 1) * width] = context[
                member * rows : (member + 1) * rows
            ]


def decode_attention(place, queries, lengths, pairs):
    rows, columns = queries.shape
    units = columns // (GROUP * HEAD_WIDTH)
    block_rows, block_columns = pairs[0].shape
    blocks = len(pairs)
    lanes = jnp.tile(lengths, GROUP)[None, :]
    scores = rows * blocks * block_rows * columns // HEAD_WIDTH
    vmem = pl.BlockSpec(memory_space=pltpu.VMEM)
    return pl.pallas_call(
        decode_kernel,
        out_shape=jax.ShapeDtypeStruct(queries.shape, queries.dtype),
        in_specs=[pl.BlockSpec(memory_space=pltpu.SMEM), vmem, vmem]
        + [pl.BlockSpec(memory_space=pl.ANY)] * blocks,
        out_specs=vmem,
        scratch_shapes=[
            pltpu.VMEM((blocks, block_rows, block_columns), jnp.bfloat16),
            pltpu.VMEM((units, rows * GROUP, 2 * HEAD_WIDTH), jnp.bfloat16),
            pltpu.VMEM((units, HEAD_WIDTH, rows * GROUP), jnp.float32),
            pltpu.VMEM((units, 8, rows * GROUP), jnp.float32),
            pltpu.SemaphoreType.DMA((blocks,)),
        ],
        compiler_params=pltpu.CompilerParams(vmem_limit_bytes=60 * MIB),
        cost_estimate=pl.CostEstimate(
            flops=4 * scores * HEAD_WIDTH,
            bytes_accessed=2 * blocks * block_rows * block_columns,
            transcendentals=scores,
        ),
        name="decode",
    )(place, queries, lanes, *pairs)


def rotate(array, distance):
    count = lax.axis_size("ctx")
    return lax.ppermute(array, "ctx", [(i, (i + distance) % count) for i in range(count)])


def swap(array):
    return lax.ppermute(array, "grp", [(0, 1), (1, 0)])


def reduce_over_heads(partial):
    count = lax.axis_size("head")
    me = lax.axis_index("head")
    rows = partial.shape[0] // count

    def piece(number):
        return lax.dynamic_slice_in_dim(partial, number * rows, rows, 0)

    power_of_two = count & (count - 1) == 0
    total = piece(me).astype(jnp.float32)
    for step in range(1, count):
        if power_of_two:
            target, pairs = me ^ step, [(i, i ^ step) for i in range(count)]
        else:
            target = (me + step) % count
            pairs = [(i, (i + step) % count) for i in range(count)]
        total += lax.ppermute(piece(target), "head", pairs).astype(jnp.float32)
    return total.astype(partial.dtype)


def local(
    prompt_queries,
    rotated_prompt_keys,
    prompt_value_rows,
    continuation_queries,
    prefix_len,
    out_weight,
):
    chips = lax.axis_size("ctx")
    chip, core = lax.axis_index("ctx"), lax.axis_index("grp")
    own = jnp.concatenate([rotated_prompt_keys, prompt_value_rows], axis=1)
    own_rows = continuation_queries.shape[0]
    my_index = chip * 2 + core
    lengths = lax.dynamic_slice_in_dim(prefix_len, my_index * own_rows, own_rows, 0)
    place = jnp.stack([chip, core]).astype(jnp.int32)

    pairs = [(own, swap(own))]
    moving = rotate(own, 1)
    state = None
    for hop in range(1, chips):
        arrived = moving
        if hop < chips - 1:
            moving = rotate(arrived, 1)
        pairs.append((arrived, swap(arrived)))
        if hop == 1:
            state = prompt_part(
                jnp.stack([core, chip >= 1]), prompt_queries, own, [pairs[0][1:], pairs[1]], None
            )
            moving, state = lax.optimization_barrier((moving, state))

    context = decode_attention(
        place, continuation_queries, lengths, [array for pair in pairs for array in pair]
    )
    spread = [context] + [rotate(context, distance) for distance in range(1, chips)]
    prompt_context = prompt_part(
        jnp.stack([chip >= hop for hop in range(2, chips)]), prompt_queries, None, pairs[2:], state
    )
    prompt_context, spread = lax.optimization_barrier((prompt_context, spread))
    stacked = jnp.concatenate([jnp.stack(spread[::-1])] * 2)
    same_core = lax.dynamic_slice_in_dim(stacked, chips - 1 - chip, chips, 0)
    other_core = swap(same_core)
    gathered = jnp.where(
        core == 0,
        jnp.stack([same_core, other_core], axis=1),
        jnp.stack([other_core, same_core], axis=1),
    ).reshape(chips * 2 * own_rows, -1)
    partial = jnp.dot(gathered, out_weight, preferred_element_type=jnp.float32)
    mixed = reduce_over_heads(partial.astype(jnp.bfloat16))
    return (prompt_context, mixed)


def solution(mesh):
    in_specs = (
        P(("ctx", "grp"), "head"),
        P(("ctx", "grp"), "head"),
        P(("ctx", "grp"), "head"),
        P(("ctx", "grp"), "head"),
        P(),
        P("head", ("ctx", "grp")),
    )
    out_specs = (P(("ctx", "grp"), "head"), P("head", ("ctx", "grp")))
    return jax.shard_map(local, mesh=mesh, in_specs=in_specs, out_specs=out_specs, check_vma=False)
```

```python
import functools
import math

import jax
import jax.numpy as jnp
from jax import lax
from jax.experimental import pallas as pl
from jax.experimental.pallas import tpu as pltpu
from jax.sharding import PartitionSpec as P

QUERY_HEADS = 64
KEY_VALUE_HEADS = 8
HEAD_WIDTH = 128
GROUP = QUERY_HEADS // KEY_VALUE_HEADS
UNITS = GROUP // 2

NEG = -1e30
SCALE = HEAD_WIDTH ** -0.5 * math.log2(math.e)
BOUND = 2.0**64
MIB = 1024 * 1024


def split_scaled(rows):
    scaled = rows.astype(jnp.float32) * SCALE
    high = scaled.astype(jnp.bfloat16)
    low = (scaled - high.astype(jnp.float32)).astype(jnp.bfloat16)
    return high, low


def score_tile(keys, queries):
    return lax.dot_general(
        jnp.concatenate([keys, keys], axis=1),
        queries,
        (((1,), (1,)), ((), ())),
        preferred_element_type=jnp.float32,
    )


def row_sums(powers):
    return jnp.sum(powers.reshape(-1, 8, powers.shape[1]), axis=0)


def pipelined(items, first, second, third):
    ahead = first(items[0])
    behind = None
    for place, item in enumerate(items):
        following = first(items[place + 1]) if place + 1 < len(items) else None
        if behind is not None:
            third(items[place - 1], behind)
        behind = second(item, ahead)
        ahead = following
    third(items[-1], behind)


def fill_split(q_ref, split_ref):
    for unit in range(split_ref.shape[0]):
        columns = slice(unit * HEAD_WIDTH, (unit + 1) * HEAD_WIDTH)
        high, low = split_scaled(q_ref[:, columns])
        split_ref[unit, :, :HEAD_WIDTH] = high
        split_ref[unit, :, HEAD_WIDTH:] = low


def later_blocks(key_refs, value_refs, split_ref, old, new):
    acc_old, sum_old, max_old = old
    acc_new, sum_new, max_new = new
    units = split_ref.shape[0]
    values = [ref[...].T for ref in value_refs]
    max_new[...] = max_old[...]

    def score(item):
        block, unit = item
        return score_tile(key_refs[block][...], split_ref[unit])

    def power(item, scores):
        block, unit = item
        powers = jnp.exp2(scores - max_old[unit])
        earlier = (sum_old if block == 0 else sum_new)[unit]
        sum_new[unit] = earlier + row_sums(powers)
        return powers.astype(jnp.bfloat16)

    def weigh(item, powers):
        block, unit = item
        earlier = (acc_old if block == 0 else acc_new)[unit]
        acc_new[unit] = earlier + jnp.dot(
            values[block], powers, preferred_element_type=jnp.float32
        )

    pipelined(
        [(block, unit) for block in range(len(key_refs)) for unit in range(units)],
        score,
        power,
        weigh,
    )

    @pl.when(jnp.max(sum_new[...]) > BOUND)
    def _():
        def one(unit, carry):
            acc, total, top = acc_old[unit], sum_old[unit], max_old[unit]
            for key_ref, value in zip(key_refs, values):
                scores = score_tile(key_ref[...], split_ref[unit])
                raised = jnp.maximum(top, jnp.max(scores, axis=0, keepdims=True))
                powers = jnp.exp2(scores - raised)
                factor = jnp.exp2(top - raised)
                total = total * factor + row_sums(powers)
                acc = acc * factor + jnp.dot(
                    value, powers.astype(jnp.bfloat16), preferred_element_type=jnp.float32
                )
                top = raised
            acc_new[unit], sum_new[unit], max_new[unit] = acc, total, top
            return carry

        lax.fori_loop(0, units, one, 0)


def write_context(o_ref, acc_ref, sum_ref):
    for unit in range(acc_ref.shape[0]):
        total = jnp.sum(sum_ref[unit], axis=0, keepdims=True)
        o_ref[:, unit * HEAD_WIDTH : (unit + 1) * HEAD_WIDTH] = (
            (acc_ref[unit] / total).T.astype(o_ref.dtype)
        )


def begin_kernel(q_ref, k_ref, v_ref, ko_ref, vo_ref, *refs):
    new, split_ref, old = refs[:3], refs[3], refs[4:]
    acc_own, sum_own, max_own = old
    fill_split(q_ref, split_ref)
    values = v_ref[...].T

    def score(unit):
        scores = score_tile(k_ref[...], split_ref[unit])
        key_at = lax.broadcasted_iota(jnp.int32, scores.shape, 0)
        row_at = lax.broadcasted_iota(jnp.int32, scores.shape, 1)
        return jnp.where(key_at <= row_at, scores, NEG)

    def power(unit, scores):
        top = jnp.max(scores, axis=0, keepdims=True)
        powers = jnp.exp2(scores - top)
        max_own[unit] = top
        sum_own[unit] = row_sums(powers)
        return powers.astype(jnp.bfloat16)

    def weigh(unit, powers):
        acc_own[unit] = jnp.dot(values, powers, preferred_element_type=jnp.float32)

    pipelined(list(range(split_ref.shape[0])), score, power, weigh)
    applies = lax.axis_index("grp") > 0

    @pl.when(jnp.logical_not(applies))
    def _():
        for source, target in zip(old, new):
            target[...] = source[...]

    @pl.when(applies)
    def _():
        later_blocks([ko_ref], [vo_ref], split_ref, old, new)


def hop_kernel(hop, ends, q_ref, k_ref, v_ref, ko_ref, vo_ref, *refs):
    old, refs = refs[:3], refs[3:]
    if ends:
        o_ref, split_ref, new = refs[0], refs[1], refs[2:]
    else:
        new, split_ref = refs[:3], refs[3]
    applies = lax.axis_index("ctx") >= hop

    @pl.when(jnp.logical_not(applies))
    def _():
        if ends:
            write_context(o_ref, *old[:2])
        else:
            for source, target in zip(old, new):
                target[...] = source[...]

    @pl.when(applies)
    def _():
        fill_split(q_ref, split_ref)
        later_blocks([k_ref, ko_ref], [v_ref, vo_ref], split_ref, old, new)
        if ends:
            write_context(o_ref, *new[:2])


def prompt_part(queries, pair, hop, ends, state):
    rows, columns = queries.shape
    heads = columns // HEAD_WIDTH
    mine, other = pair
    heads_kv = mine.shape[1] // (2 * HEAD_WIDTH)
    steps_each = GROUP // UNITS
    wide = pl.BlockSpec((rows, UNITS * HEAD_WIDTH), lambda h: (0, h))
    key_spec = pl.BlockSpec((rows, HEAD_WIDTH), lambda h: (0, h // steps_each))
    value_spec = pl.BlockSpec((rows, HEAD_WIDTH), lambda h: (0, heads_kv + h // steps_each))
    depths = (HEAD_WIDTH, 8, 1)
    state_specs = [pl.BlockSpec((UNITS, depth, rows), lambda h: (h, 0, 0)) for depth in depths]
    held = [pltpu.VMEM((UNITS, depth, rows), jnp.float32) for depth in depths]
    scratch = [pltpu.VMEM((UNITS, rows, 2 * HEAD_WIDTH), jnp.bfloat16)]
    if hop == 0 or ends:
        scratch += held
    if ends:
        out_specs, out_shape = wide, jax.ShapeDtypeStruct(queries.shape, queries.dtype)
    else:
        out_specs = state_specs
        out_shape = [jax.ShapeDtypeStruct((heads, depth, rows), jnp.float32) for depth in depths]
    scores = 2 * rows * rows * heads
    return pl.pallas_call(
        begin_kernel if hop == 0 else functools.partial(hop_kernel, hop, ends),
        out_shape=out_shape,
        grid_spec=pl.GridSpec(
            grid=(heads // UNITS,),
            in_specs=[wide] + [key_spec, value_spec] * 2 + (state_specs if hop else []),
            out_specs=out_specs,
            scratch_shapes=scratch,
        ),
        compiler_params=pltpu.CompilerParams(vmem_limit_bytes=60 * MIB),
        cost_estimate=pl.CostEstimate(
            flops=4 * scores * HEAD_WIDTH, bytes_accessed=8 * queries.size, transcendentals=scores
        ),
        name="prompt_%d" % hop,
    )(queries, mine, mine, other, other, *(state or ()))


def decode_kernel(q_ref, len_ref, *refs):
    slots = len(refs) - 6
    pairs = refs[:slots]
    o_ref, kv_ref, split_ref, acc_ref, sum_ref, sem = refs[slots:]
    rows = q_ref.shape[0]
    units = split_ref.shape[0]
    blocks, block_rows = kv_ref.shape[:2]
    width = HEAD_WIDTH
    chip, core = lax.axis_index("ctx"), lax.axis_index("grp")
    for slot in range(slots):
        at = chip - slot // 2
        at = jnp.where(at < 0, at + slots // 2, at)
        block = 2 * at + (core if slot % 2 == 0 else 1 - core)
        pltpu.make_async_copy(pairs[slot], kv_ref.at[block], sem.at[block]).start()
    for unit in range(units):
        for member in range(GROUP):
            head = unit * GROUP + member
            high, low = split_scaled(q_ref[:, head * width : (head + 1) * width])
            split_ref[unit, member * rows : (member + 1) * rows, :width] = high
            split_ref[unit, member * rows : (member + 1) * rows, width:] = low
    lengths = len_ref[...]

    def masked(block, unit):
        columns = pl.ds(pl.multiple_of(unit * width, width), width)
        scores = score_tile(kv_ref[block, :, columns], split_ref[unit])
        key_at = lax.broadcasted_iota(jnp.int32, scores.shape, 0)
        return jnp.where(key_at < lengths - block * block_rows, scores, NEG)

    def values_of(block, unit):
        columns = pl.ds(pl.multiple_of((units + unit) * width, width), width)
        return kv_ref[block, :, columns].T

    tops = [None] * units

    def first(item):
        block, unit = item
        if unit == 0:
            pltpu.make_async_copy(pairs[0], kv_ref.at[block], sem.at[block]).wait()
        return masked(block, unit), values_of(block, unit)

    def second(item, ahead):
        (block, unit), (scores, values) = item, ahead
        if block == 0:
            tops[unit] = jnp.max(scores, axis=0, keepdims=True)
        powers = jnp.exp2(scores - tops[unit])
        sums = row_sums(powers)
        sum_ref[unit] = sums if block == 0 else sum_ref[unit] + sums
        return powers.astype(jnp.bfloat16), values

    def third(item, behind):
        (block, unit), (powers, values) = item, behind
        added = jnp.dot(values, powers, preferred_element_type=jnp.float32)
        acc_ref[unit] = added if block == 0 else acc_ref[unit] + added

    items = [(block, unit) for block in range(blocks) for unit in range(units)]
    pipelined(items, first, second, third)

    @pl.when(jnp.max(sum_ref[...]) > BOUND)
    def _():
        def one(unit, carry):
            acc_ref[unit] = jnp.zeros(acc_ref.shape[1:], jnp.float32)
            sum_ref[unit] = jnp.zeros(sum_ref.shape[1:], jnp.float32)

            def visit(block, top):
                scores = masked(block, unit)
                raised = jnp.maximum(top, jnp.max(scores, axis=0, keepdims=True))
                powers = jnp.exp2(scores - raised)
                factor = jnp.exp2(top - raised)
                sum_ref[unit] = sum_ref[unit] * factor + row_sums(powers)
                acc_ref[unit] = acc_ref[unit] * factor + jnp.dot(
                    values_of(block, unit),
                    powers.astype(jnp.bfloat16),
                    preferred_element_type=jnp.float32,
                )
                return raised

            lax.fori_loop(0, blocks, visit, jnp.full(lengths.shape, NEG, jnp.float32))
            return carry

        lax.fori_loop(0, units, one, 0)

    for unit in range(units):
        total = jnp.sum(sum_ref[unit], axis=0, keepdims=True)
        context = (acc_ref[unit] / total).T.astype(o_ref.dtype)
        for member in range(GROUP):
            head = unit * GROUP + member
            o_ref[:, head * width : (head + 1) * width] = context[
                member * rows : (member + 1) * rows
            ]


def decode_attention(queries, lanes, pairs):
    rows, columns = queries.shape
    units = columns // (GROUP * HEAD_WIDTH)
    block_rows, block_columns = pairs[0].shape
    blocks = len(pairs)
    scores = rows * blocks * block_rows * columns // HEAD_WIDTH
    vmem = pl.BlockSpec(memory_space=pltpu.VMEM)
    return pl.pallas_call(
        decode_kernel,
        out_shape=jax.ShapeDtypeStruct(queries.shape, queries.dtype),
        in_specs=[vmem, vmem]
        + [pl.BlockSpec(memory_space=pl.ANY)] * blocks,
        out_specs=vmem,
        scratch_shapes=[
            pltpu.VMEM((blocks, block_rows, block_columns), jnp.bfloat16),
            pltpu.VMEM((units, rows * GROUP, 2 * HEAD_WIDTH), jnp.bfloat16),
            pltpu.VMEM((units, HEAD_WIDTH, rows * GROUP), jnp.float32),
            pltpu.VMEM((units, 8, rows * GROUP), jnp.float32),
            pltpu.SemaphoreType.DMA((blocks,)),
        ],
        compiler_params=pltpu.CompilerParams(vmem_limit_bytes=60 * MIB),
        cost_estimate=pl.CostEstimate(
            flops=4 * scores * HEAD_WIDTH,
            bytes_accessed=2 * blocks * block_rows * block_columns,
            transcendentals=scores,
        ),
        name="decode",
    )(queries, lanes, *pairs)


def rotate(array, distance):
    count = lax.axis_size("ctx")
    return lax.ppermute(array, "ctx", [(i, (i + distance) % count) for i in range(count)])


def swap(array):
    return lax.ppermute(array, "grp", [(0, 1), (1, 0)])


def reduce_over_heads(piece):
    count = lax.axis_size("head")
    me = lax.axis_index("head")
    power_of_two = count & (count - 1) == 0
    terms = [piece(me)]
    for step in range(1, count):
        if power_of_two:
            target, pairs = me ^ step, [(i, i ^ step) for i in range(count)]
        else:
            target = (me + step) % count
            pairs = [(i, (i + step) % count) for i in range(count)]
        terms.append(lax.ppermute(piece(target), "head", pairs))
    return terms


def total_of(terms):
    return sum(term.astype(jnp.float32) for term in terms).astype(jnp.bfloat16)


def project(spread, out_weight):
    chips, rows, columns = spread.shape
    count = lax.axis_size("head")
    chip, core = lax.axis_index("ctx"), lax.axis_index("grp")

    def share(context):
        partial = jnp.dot(
            context.reshape(-1, columns), out_weight, preferred_element_type=jnp.float32
        )
        return partial.astype(jnp.bfloat16).reshape(chips, rows, -1)

    def in_order(mine, other):
        both = jnp.where(
            core == 0, jnp.stack([mine, other], axis=1), jnp.stack([other, mine], axis=1)
        )
        return both.reshape(-1, both.shape[-1])

    def one(partial, slot):
        return lax.dynamic_index_in_dim(partial, slot % chips, 0, keepdims=False)

    swapped = swap(spread)
    if chips == count:
        sums = []
        for context in (spread, swapped):
            partial = share(context)
            sums.append(reduce_over_heads(lambda j: one(partial, chip + chips - j)))
        mine, other = total_of(sums[0]), total_of(sums[1])
        return in_order(mine[None], other[None])

    def by_chip(partial):
        return jnp.stack([one(partial, chip + chips - c) for c in range(chips)])

    partial = in_order(by_chip(share(spread)), by_chip(share(swapped)))
    kept = partial.shape[0] // count
    return total_of(
        reduce_over_heads(lambda j: lax.dynamic_slice_in_dim(partial, j * kept, kept, 0))
    )


def local(
    prompt_queries,
    rotated_prompt_keys,
    prompt_value_rows,
    continuation_queries,
    prefix_len,
    out_weight,
):
    chips = lax.axis_size("ctx")
    chip, core = lax.axis_index("ctx"), lax.axis_index("grp")
    own = jnp.concatenate([rotated_prompt_keys, prompt_value_rows], axis=1)
    own_rows = continuation_queries.shape[0]
    my_index = chip * 2 + core
    lengths = lax.dynamic_slice_in_dim(prefix_len, my_index * own_rows, own_rows, 0)
    lanes = jnp.tile(lengths, GROUP)[None, :]

    pairs = [(own, swap(own))]
    moving = rotate(own, 1)
    state = prompt_part(prompt_queries, pairs[0], 0, False, None)
    moving, state, lanes = lax.optimization_barrier((moving, state, lanes))
    for hop in range(1, chips):
        arrived = moving
        if hop < chips - 1:
            moving = rotate(arrived, 1)
        pairs.append((arrived, swap(arrived)))
        if hop < chips - 1:
            state = prompt_part(prompt_queries, pairs[hop], hop, False, state)
            moving, state = lax.optimization_barrier((moving, state))

    context = decode_attention(
        continuation_queries, lanes, [array for pair in pairs for array in pair]
    )
    spread = [context] + [rotate(context, distance) for distance in range(1, chips)]
    prompt_context = prompt_part(prompt_queries, pairs[-1], chips - 1, True, state)
    prompt_context, spread = lax.optimization_barrier((prompt_context, spread))
    return (prompt_context, project(jnp.stack(spread), out_weight))


def solution(mesh):
    in_specs = (
        P(("ctx", "grp"), "head"),
        P(("ctx", "grp"), "head"),
        P(("ctx", "grp"), "head"),
        P(("ctx", "grp"), "head"),
        P(),
        P("head", ("ctx", "grp")),
    )
    out_specs = (P(("ctx", "grp"), "head"), P("head", ("ctx", "grp")))
    return jax.shard_map(local, mesh=mesh, in_specs=in_specs, out_specs=out_specs, check_vma=False)
```

```python
import functools
import math

import jax
import jax.numpy as jnp
from jax import lax
from jax.experimental import pallas as pl
from jax.experimental.pallas import tpu as pltpu
from jax.sharding import PartitionSpec as P

QUERY_HEADS = 64
KEY_VALUE_HEADS = 8
HEAD_WIDTH = 128
GROUP = QUERY_HEADS // KEY_VALUE_HEADS
UNITS = GROUP // 2

NEG = -1e30
SCALE = HEAD_WIDTH ** -0.5 * math.log2(math.e)
BOUND = 2.0**64
MIB = 1024 * 1024


def split_scaled(rows):
    scaled = rows.astype(jnp.float32) * SCALE
    high = scaled.astype(jnp.bfloat16)
    low = (scaled - high.astype(jnp.float32)).astype(jnp.bfloat16)
    return high, low


def score_tile(keys, queries):
    return lax.dot_general(
        jnp.concatenate([keys, keys], axis=1),
        queries,
        (((1,), (1,)), ((), ())),
        preferred_element_type=jnp.float32,
    )


def row_sums(powers):
    return jnp.sum(powers.reshape(-1, 8, powers.shape[1]), axis=0)


def pipelined(items, first, second, third):
    ahead = first(items[0])
    behind = None
    for place, item in enumerate(items):
        following = first(items[place + 1]) if place + 1 < len(items) else None
        if behind is not None:
            third(items[place - 1], behind)
        behind = second(item, ahead)
        ahead = following
    third(items[-1], behind)


def fill_split(q_ref, split_ref):
    for unit in range(split_ref.shape[0]):
        columns = slice(unit * HEAD_WIDTH, (unit + 1) * HEAD_WIDTH)
        high, low = split_scaled(q_ref[:, columns])
        split_ref[unit, :, :HEAD_WIDTH] = high
        split_ref[unit, :, HEAD_WIDTH:] = low


def later_blocks(key_refs, value_refs, split_ref, old, new):
    acc_old, sum_old, max_old = old
    acc_new, sum_new, max_new = new
    units = split_ref.shape[0]
    values = [ref[...].T for ref in value_refs]
    max_new[...] = max_old[...]

    def score(item):
        block, unit = item
        return score_tile(key_refs[block][...], split_ref[unit])

    def power(item, scores):
        block, unit = item
        powers = jnp.exp2(scores - max_old[unit])
        earlier = (sum_old if block == 0 else sum_new)[unit]
        sum_new[unit] = earlier + row_sums(powers)
        return powers.astype(jnp.bfloat16)

    def weigh(item, powers):
        block, unit = item
        earlier = (acc_old if block == 0 else acc_new)[unit]
        acc_new[unit] = earlier + jnp.dot(
            values[block], powers, preferred_element_type=jnp.float32
        )

    pipelined(
        [(block, unit) for block in range(len(key_refs)) for unit in range(units)],
        score,
        power,
        weigh,
    )

    @pl.when(jnp.max(sum_new[...]) > BOUND)
    def _():
        def one(unit, carry):
            acc, total, top = acc_old[unit], sum_old[unit], max_old[unit]
            for key_ref, value in zip(key_refs, values):
                scores = score_tile(key_ref[...], split_ref[unit])
                raised = jnp.maximum(top, jnp.max(scores, axis=0, keepdims=True))
                powers = jnp.exp2(scores - raised)
                factor = jnp.exp2(top - raised)
                total = total * factor + row_sums(powers)
                acc = acc * factor + jnp.dot(
                    value, powers.astype(jnp.bfloat16), preferred_element_type=jnp.float32
                )
                top = raised
            acc_new[unit], sum_new[unit], max_new[unit] = acc, total, top
            return carry

        lax.fori_loop(0, units, one, 0)


def write_context(o_ref, acc_ref, sum_ref):
    for unit in range(acc_ref.shape[0]):
        total = jnp.sum(sum_ref[unit], axis=0, keepdims=True)
        o_ref[:, unit * HEAD_WIDTH : (unit + 1) * HEAD_WIDTH] = (
            (acc_ref[unit] / total).T.astype(o_ref.dtype)
        )


def begin_kernel(q_ref, k_ref, v_ref, ko_ref, vo_ref, *refs):
    new, split_ref, old = refs[:3], refs[3], refs[4:]
    acc_own, sum_own, max_own = old
    fill_split(q_ref, split_ref)
    values = v_ref[...].T

    def score(unit):
        scores = score_tile(k_ref[...], split_ref[unit])
        key_at = lax.broadcasted_iota(jnp.int32, scores.shape, 0)
        row_at = lax.broadcasted_iota(jnp.int32, scores.shape, 1)
        return jnp.where(key_at <= row_at, scores, NEG)

    def power(unit, scores):
        top = jnp.max(scores, axis=0, keepdims=True)
        powers = jnp.exp2(scores - top)
        max_own[unit] = top
        sum_own[unit] = row_sums(powers)
        return powers.astype(jnp.bfloat16)

    def weigh(unit, powers):
        acc_own[unit] = jnp.dot(values, powers, preferred_element_type=jnp.float32)

    pipelined(list(range(split_ref.shape[0])), score, power, weigh)
    applies = lax.axis_index("grp") > 0

    @pl.when(jnp.logical_not(applies))
    def _():
        for source, target in zip(old, new):
            target[...] = source[...]

    @pl.when(applies)
    def _():
        later_blocks([ko_ref], [vo_ref], split_ref, old, new)


def hop_kernel(hop, ends, q_ref, k_ref, v_ref, ko_ref, vo_ref, *refs):
    old, refs = refs[:3], refs[3:]
    if ends:
        o_ref, split_ref, new = refs[0], refs[1], refs[2:]
    else:
        new, split_ref = refs[:3], refs[3]
    applies = lax.axis_index("ctx") >= hop

    @pl.when(jnp.logical_not(applies))
    def _():
        if ends:
            write_context(o_ref, *old[:2])
        else:
            for source, target in zip(old, new):
                target[...] = source[...]

    @pl.when(applies)
    def _():
        fill_split(q_ref, split_ref)
        later_blocks([k_ref, ko_ref], [v_ref, vo_ref], split_ref, old, new)
        if ends:
            write_context(o_ref, *new[:2])


def prompt_part(queries, pair, hop, ends, state):
    rows, columns = queries.shape
    heads = columns // HEAD_WIDTH
    mine, other = pair
    heads_kv = mine.shape[1] // (2 * HEAD_WIDTH)
    steps_each = GROUP // UNITS
    wide = pl.BlockSpec((rows, UNITS * HEAD_WIDTH), lambda h: (0, h))
    key_spec = pl.BlockSpec((rows, HEAD_WIDTH), lambda h: (0, h // steps_each))
    value_spec = pl.BlockSpec((rows, HEAD_WIDTH), lambda h: (0, heads_kv + h // steps_each))
    depths = (HEAD_WIDTH, 8, 1)
    state_specs = [pl.BlockSpec((UNITS, depth, rows), lambda h: (h, 0, 0)) for depth in depths]
    held = [pltpu.VMEM((UNITS, depth, rows), jnp.float32) for depth in depths]
    scratch = [pltpu.VMEM((UNITS, rows, 2 * HEAD_WIDTH), jnp.bfloat16)]
    if hop == 0 or ends:
        scratch += held
    if ends:
        out_specs, out_shape = wide, jax.ShapeDtypeStruct(queries.shape, queries.dtype)
    else:
        out_specs = state_specs
        out_shape = [jax.ShapeDtypeStruct((heads, depth, rows), jnp.float32) for depth in depths]
    scores = 2 * rows * rows * heads
    return pl.pallas_call(
        begin_kernel if hop == 0 else functools.partial(hop_kernel, hop, ends),
        out_shape=out_shape,
        grid_spec=pl.GridSpec(
            grid=(heads // UNITS,),
            in_specs=[wide] + [key_spec, value_spec] * 2 + (state_specs if hop else []),
            out_specs=out_specs,
            scratch_shapes=scratch,
        ),
        compiler_params=pltpu.CompilerParams(vmem_limit_bytes=20 * MIB),
        cost_estimate=pl.CostEstimate(
            flops=4 * scores * HEAD_WIDTH, bytes_accessed=8 * queries.size, transcendentals=scores
        ),
        name="prompt_%d" % hop,
    )(queries, mine, mine, other, other, *(state or ()))


def decode_kernel(q_ref, len_ref, *refs):
    slots = len(refs) - 5
    pairs = refs[:slots]
    o_ref, first_ref, split_ref, acc_ref, sum_ref = refs[slots:]
    rows = q_ref.shape[0]
    units = split_ref.shape[0]
    block_rows = first_ref.shape[0]
    width = HEAD_WIDTH
    chip, core = lax.axis_index("ctx"), lax.axis_index("grp")
    starts = []
    for slot in range(slots):
        at = chip - slot // 2
        at = jnp.where(at < 0, at + slots // 2, at)
        block = 2 * at + (core if slot % 2 == 0 else 1 - core)
        starts.append(block * block_rows)

        @pl.when(block == 0)
        def _():
            first_ref[...] = pairs[slot][:, : units * width]

    for unit in range(units):
        for member in range(GROUP):
            head = unit * GROUP + member
            high, low = split_scaled(q_ref[:, head * width : (head + 1) * width])
            split_ref[unit, member * rows : (member + 1) * rows, :width] = high
            split_ref[unit, member * rows : (member + 1) * rows, width:] = low
    lengths = len_ref[...]

    def masked(keys, start, unit):
        scores = score_tile(keys, split_ref[unit])
        key_at = lax.broadcasted_iota(jnp.int32, scores.shape, 0)
        return jnp.where(key_at < lengths - start, scores, NEG)

    def key_columns(unit):
        return pl.ds(pl.multiple_of(unit * width, width), width)

    def value_columns(unit):
        return pl.ds(pl.multiple_of((units + unit) * width, width), width)

    tops = [
        jnp.max(masked(first_ref[:, key_columns(unit)], 0, unit), axis=0, keepdims=True)
        for unit in range(units)
    ]

    def first(item):
        slot, unit = item
        return masked(pairs[slot][:, key_columns(unit)], starts[slot], unit)

    def second(item, scores):
        slot, unit = item
        powers = jnp.exp2(scores - tops[unit])
        sums = row_sums(powers)
        sum_ref[unit] = sums if slot == 0 else sum_ref[unit] + sums
        return powers.astype(jnp.bfloat16)

    def third(item, powers):
        slot, unit = item
        values = pairs[slot][:, value_columns(unit)].T
        added = jnp.dot(values, powers, preferred_element_type=jnp.float32)
        acc_ref[unit] = added if slot == 0 else acc_ref[unit] + added

    pipelined(
        [(slot, unit) for slot in range(slots) for unit in range(units)], first, second, third
    )

    @pl.when(jnp.max(sum_ref[...]) > BOUND)
    def _():
        def one(unit, carry):
            acc = jnp.zeros(acc_ref.shape[1:], jnp.float32)
            total = jnp.zeros(sum_ref.shape[1:], jnp.float32)
            top = jnp.full(lengths.shape, NEG, jnp.float32)
            for slot in range(slots):
                scores = masked(pairs[slot][:, key_columns(unit)], starts[slot], unit)
                raised = jnp.maximum(top, jnp.max(scores, axis=0, keepdims=True))
                powers = jnp.exp2(scores - raised)
                factor = jnp.exp2(top - raised)
                total = total * factor + row_sums(powers)
                acc = acc * factor + jnp.dot(
                    pairs[slot][:, value_columns(unit)].T,
                    powers.astype(jnp.bfloat16),
                    preferred_element_type=jnp.float32,
                )
                top = raised
            acc_ref[unit], sum_ref[unit] = acc, total
            return carry

        lax.fori_loop(0, units, one, 0)

    for unit in range(units):
        total = jnp.sum(sum_ref[unit], axis=0, keepdims=True)
        context = (acc_ref[unit] / total).T.astype(o_ref.dtype)
        for member in range(GROUP):
            head = unit * GROUP + member
            o_ref[:, head * width : (head + 1) * width] = context[
                member * rows : (member + 1) * rows
            ]


def decode_attention(queries, lanes, pairs):
    rows, columns = queries.shape
    units = columns // (GROUP * HEAD_WIDTH)
    block_rows, block_columns = pairs[0].shape
    blocks = len(pairs)
    scores = rows * blocks * block_rows * columns // HEAD_WIDTH
    vmem = pl.BlockSpec(memory_space=pltpu.VMEM)
    return pl.pallas_call(
        decode_kernel,
        out_shape=jax.ShapeDtypeStruct(queries.shape, queries.dtype),
        in_specs=[vmem] * (2 + blocks),
        out_specs=vmem,
        scratch_shapes=[
            pltpu.VMEM((block_rows, units * HEAD_WIDTH), jnp.bfloat16),
            pltpu.VMEM((units, rows * GROUP, 2 * HEAD_WIDTH), jnp.bfloat16),
            pltpu.VMEM((units, HEAD_WIDTH, rows * GROUP), jnp.float32),
            pltpu.VMEM((units, 8, rows * GROUP), jnp.float32),
        ],
        compiler_params=pltpu.CompilerParams(vmem_limit_bytes=20 * MIB),
        cost_estimate=pl.CostEstimate(
            flops=4 * scores * HEAD_WIDTH,
            bytes_accessed=2 * blocks * block_rows * block_columns,
            transcendentals=scores,
        ),
        name="decode",
    )(queries, lanes, *pairs)


def rotate(array, distance):
    count = lax.axis_size("ctx")
    return lax.ppermute(array, "ctx", [(i, (i + distance) % count) for i in range(count)])


def swap(array):
    return lax.ppermute(array, "grp", [(0, 1), (1, 0)])


def reduce_over_heads(piece):
    count = lax.axis_size("head")
    me = lax.axis_index("head")
    power_of_two = count & (count - 1) == 0
    terms = [piece(me)]
    for step in range(1, count):
        if power_of_two:
            target, pairs = me ^ step, [(i, i ^ step) for i in range(count)]
        else:
            target = (me + step) % count
            pairs = [(i, (i + step) % count) for i in range(count)]
        terms.append(lax.ppermute(piece(target), "head", pairs))
    return terms


def total_of(terms):
    return sum(term.astype(jnp.float32) for term in terms).astype(jnp.bfloat16)


def project(spread, out_weight):
    chips, rows, columns = spread.shape
    count = lax.axis_size("head")
    chip, core = lax.axis_index("ctx"), lax.axis_index("grp")

    def share(context):
        partial = jnp.dot(
            context.reshape(-1, columns), out_weight, preferred_element_type=jnp.float32
        )
        return partial.astype(jnp.bfloat16).reshape(chips, rows, -1)

    def in_order(mine, other):
        both = jnp.where(
            core == 0, jnp.stack([mine, other], axis=1), jnp.stack([other, mine], axis=1)
        )
        return both.reshape(-1, both.shape[-1])

    def one(partial, slot):
        return lax.dynamic_index_in_dim(partial, slot % chips, 0, keepdims=False)

    swapped = swap(spread)
    if chips == count:
        sums = []
        for context in (spread, swapped):
            partial = share(context)
            sums.append(reduce_over_heads(lambda j: one(partial, chip + chips - j)))
        mine, other = total_of(sums[0]), total_of(sums[1])
        return in_order(mine[None], other[None])

    def by_chip(partial):
        return jnp.stack([one(partial, chip + chips - c) for c in range(chips)])

    partial = in_order(by_chip(share(spread)), by_chip(share(swapped)))
    kept = partial.shape[0] // count
    return total_of(
        reduce_over_heads(lambda j: lax.dynamic_slice_in_dim(partial, j * kept, kept, 0))
    )


def local(
    prompt_queries,
    rotated_prompt_keys,
    prompt_value_rows,
    continuation_queries,
    prefix_len,
    out_weight,
):
    chips = lax.axis_size("ctx")
    chip, core = lax.axis_index("ctx"), lax.axis_index("grp")
    own = jnp.concatenate([rotated_prompt_keys, prompt_value_rows], axis=1)
    own_rows = continuation_queries.shape[0]
    my_index = chip * 2 + core
    lengths = lax.dynamic_slice_in_dim(prefix_len, my_index * own_rows, own_rows, 0)
    lanes = jnp.tile(lengths, GROUP)[None, :]

    pairs = [(own, swap(own))]
    moving = rotate(own, 1)
    state = prompt_part(prompt_queries, pairs[0], 0, False, None)
    moving, state, lanes = lax.optimization_barrier((moving, state, lanes))
    for hop in range(1, chips):
        arrived = moving
        if hop < chips - 1:
            moving = rotate(arrived, 1)
        pairs.append((arrived, swap(arrived)))
        if hop < chips - 1:
            state = prompt_part(prompt_queries, pairs[hop], hop, False, state)
            moving, state = lax.optimization_barrier((moving, state))

    context = decode_attention(
        continuation_queries, lanes, [array for pair in pairs for array in pair]
    )
    spread = [context] + [rotate(context, distance) for distance in range(1, chips)]
    prompt_context = prompt_part(prompt_queries, pairs[-1], chips - 1, True, state)
    prompt_context, spread = lax.optimization_barrier((prompt_context, spread))
    return (prompt_context, project(jnp.stack(spread), out_weight))


def solution(mesh):
    in_specs = (
        P(("ctx", "grp"), "head"),
        P(("ctx", "grp"), "head"),
        P(("ctx", "grp"), "head"),
        P(("ctx", "grp"), "head"),
        P(),
        P("head", ("ctx", "grp")),
    )
    out_specs = (P(("ctx", "grp"), "head"), P("head", ("ctx", "grp")))
    return jax.shard_map(local, mesh=mesh, in_specs=in_specs, out_specs=out_specs, check_vma=False)
```

```python
import functools
import math

import jax
import jax.numpy as jnp
from jax import lax
from jax.experimental import pallas as pl
from jax.experimental.pallas import tpu as pltpu
from jax.sharding import PartitionSpec as P

QUERY_HEADS = 64
KEY_VALUE_HEADS = 8
HEAD_WIDTH = 128
GROUP = QUERY_HEADS // KEY_VALUE_HEADS
UNITS = GROUP // 2

NEG = -1e30
SCALE = HEAD_WIDTH ** -0.5 * math.log2(math.e)
BOUND = 2.0**64
MIB = 1024 * 1024


def split_scaled(rows):
    scaled = rows.astype(jnp.float32) * SCALE
    high = scaled.astype(jnp.bfloat16)
    low = (scaled - high.astype(jnp.float32)).astype(jnp.bfloat16)
    return high, low


def score_tile(keys, queries):
    return lax.dot_general(
        jnp.concatenate([keys, keys], axis=1),
        queries,
        (((1,), (1,)), ((), ())),
        preferred_element_type=jnp.float32,
    )


def row_sums(powers):
    return jnp.sum(powers.reshape(-1, 8, powers.shape[1]), axis=0)


def pipelined(items, first, second, third):
    ahead = first(items[0])
    behind = None
    for place, item in enumerate(items):
        following = first(items[place + 1]) if place + 1 < len(items) else None
        if behind is not None:
            third(items[place - 1], behind)
        behind = second(item, ahead)
        ahead = following
    third(items[-1], behind)


def fill_split(q_ref, split_ref):
    for unit in range(split_ref.shape[0]):
        columns = slice(unit * HEAD_WIDTH, (unit + 1) * HEAD_WIDTH)
        high, low = split_scaled(q_ref[:, columns])
        split_ref[unit, :, :HEAD_WIDTH] = high
        split_ref[unit, :, HEAD_WIDTH:] = low


def later_blocks(key_refs, value_refs, split_ref, old, new):
    acc_old, sum_old, max_old = old
    acc_new, sum_new, max_new = new
    units = split_ref.shape[0]
    values = [ref[...].T for ref in value_refs]
    max_new[...] = max_old[...]

    def score(item):
        block, unit = item
        return score_tile(key_refs[block][...], split_ref[unit])

    def power(item, scores):
        block, unit = item
        powers = jnp.exp2(scores - max_old[unit])
        earlier = (sum_old if block == 0 else sum_new)[unit]
        sum_new[unit] = earlier + row_sums(powers)
        return powers.astype(jnp.bfloat16)

    def weigh(item, powers):
        block, unit = item
        earlier = (acc_old if block == 0 else acc_new)[unit]
        acc_new[unit] = earlier + jnp.dot(
            values[block], powers, preferred_element_type=jnp.float32
        )

    pipelined(
        [(block, unit) for block in range(len(key_refs)) for unit in range(units)],
        score,
        power,
        weigh,
    )

    @pl.when(jnp.max(sum_new[...]) > BOUND)
    def _():
        def one(unit, carry):
            acc, total, top = acc_old[unit], sum_old[unit], max_old[unit]
            for key_ref, value in zip(key_refs, values):
                scores = score_tile(key_ref[...], split_ref[unit])
                raised = jnp.maximum(top, jnp.max(scores, axis=0, keepdims=True))
                powers = jnp.exp2(scores - raised)
                factor = jnp.exp2(top - raised)
                total = total * factor + row_sums(powers)
                acc = acc * factor + jnp.dot(
                    value, powers.astype(jnp.bfloat16), preferred_element_type=jnp.float32
                )
                top = raised
            acc_new[unit], sum_new[unit], max_new[unit] = acc, total, top
            return carry

        lax.fori_loop(0, units, one, 0)


def write_context(o_ref, acc_ref, sum_ref):
    for unit in range(acc_ref.shape[0]):
        total = jnp.sum(sum_ref[unit], axis=0, keepdims=True)
        o_ref[:, unit * HEAD_WIDTH : (unit + 1) * HEAD_WIDTH] = (
            (acc_ref[unit] / total).T.astype(o_ref.dtype)
        )


def begin_kernel(q_ref, k_ref, v_ref, ko_ref, vo_ref, *refs):
    new, split_ref, old = refs[:3], refs[3], refs[4:]
    acc_own, sum_own, max_own = old
    fill_split(q_ref, split_ref)
    values = v_ref[...].T

    def score(unit):
        scores = score_tile(k_ref[...], split_ref[unit])
        key_at = lax.broadcasted_iota(jnp.int32, scores.shape, 0)
        row_at = lax.broadcasted_iota(jnp.int32, scores.shape, 1)
        return jnp.where(key_at <= row_at, scores, NEG)

    def power(unit, scores):
        top = jnp.max(scores, axis=0, keepdims=True)
        powers = jnp.exp2(scores - top)
        max_own[unit] = top
        sum_own[unit] = row_sums(powers)
        return powers.astype(jnp.bfloat16)

    def weigh(unit, powers):
        acc_own[unit] = jnp.dot(values, powers, preferred_element_type=jnp.float32)

    pipelined(list(range(split_ref.shape[0])), score, power, weigh)
    applies = lax.axis_index("grp") > 0

    @pl.when(jnp.logical_not(applies))
    def _():
        for source, target in zip(old, new):
            target[...] = source[...]

    @pl.when(applies)
    def _():
        later_blocks([ko_ref], [vo_ref], split_ref, old, new)


def hop_kernel(hop, ends, q_ref, k_ref, v_ref, ko_ref, vo_ref, *refs):
    old, refs = refs[:3], refs[3:]
    if ends:
        o_ref, split_ref, new = refs[0], refs[1], refs[2:]
    else:
        new, split_ref = refs[:3], refs[3]
    applies = lax.axis_index("ctx") >= hop

    @pl.when(jnp.logical_not(applies))
    def _():
        if ends:
            write_context(o_ref, *old[:2])
        else:
            for source, target in zip(old, new):
                target[...] = source[...]

    @pl.when(applies)
    def _():
        fill_split(q_ref, split_ref)
        later_blocks([k_ref, ko_ref], [v_ref, vo_ref], split_ref, old, new)
        if ends:
            write_context(o_ref, *new[:2])


def prompt_part(queries, pair, hop, ends, state):
    rows, columns = queries.shape
    heads = columns // HEAD_WIDTH
    mine, other = pair
    heads_kv = mine.shape[1] // (2 * HEAD_WIDTH)
    steps_each = GROUP // UNITS
    wide = pl.BlockSpec((rows, UNITS * HEAD_WIDTH), lambda h: (0, h))
    key_spec = pl.BlockSpec((rows, HEAD_WIDTH), lambda h: (0, h // steps_each))
    value_spec = pl.BlockSpec((rows, HEAD_WIDTH), lambda h: (0, heads_kv + h // steps_each))
    depths = (HEAD_WIDTH, 8, 1)
    state_specs = [pl.BlockSpec((UNITS, depth, rows), lambda h: (h, 0, 0)) for depth in depths]
    held = [pltpu.VMEM((UNITS, depth, rows), jnp.float32) for depth in depths]
    scratch = [pltpu.VMEM((UNITS, rows, 2 * HEAD_WIDTH), jnp.bfloat16)]
    if hop == 0 or ends:
        scratch += held
    if ends:
        out_specs, out_shape = wide, jax.ShapeDtypeStruct(queries.shape, queries.dtype)
    else:
        out_specs = state_specs
        out_shape = [jax.ShapeDtypeStruct((heads, depth, rows), jnp.float32) for depth in depths]
    scores = 2 * rows * rows * heads
    return pl.pallas_call(
        begin_kernel if hop == 0 else functools.partial(hop_kernel, hop, ends),
        out_shape=out_shape,
        grid_spec=pl.GridSpec(
            grid=(heads // UNITS,),
            in_specs=[wide] + [key_spec, value_spec] * 2 + (state_specs if hop else []),
            out_specs=out_specs,
            scratch_shapes=scratch,
        ),
        compiler_params=pltpu.CompilerParams(vmem_limit_bytes=20 * MIB),
        cost_estimate=pl.CostEstimate(
            flops=4 * scores * HEAD_WIDTH, bytes_accessed=8 * queries.size, transcendentals=scores
        ),
        name="prompt_%d" % hop,
    )(queries, mine, mine, other, other, *(state or ()))


def decode_kernel(q_ref, len_ref, *refs):
    slots = len(refs) - 5
    pairs = refs[:slots]
    o_ref, first_ref, split_ref, acc_ref, sum_ref = refs[slots:]
    rows = q_ref.shape[0]
    units = split_ref.shape[0]
    block_rows = first_ref.shape[0]
    width = HEAD_WIDTH
    chip, core = lax.axis_index("ctx"), lax.axis_index("grp")
    starts = []
    for slot in range(slots):
        at = chip - slot // 2
        at = jnp.where(at < 0, at + slots // 2, at)
        block = 2 * at + (core if slot % 2 == 0 else 1 - core)
        starts.append(block * block_rows)

        @pl.when(block == 0)
        def _():
            first_ref[...] = pairs[slot][:, : units * width]

    for unit in range(units):
        for member in range(GROUP):
            head = unit * GROUP + member
            high, low = split_scaled(q_ref[:, head * width : (head + 1) * width])
            split_ref[unit, member * rows : (member + 1) * rows, :width] = high
            split_ref[unit, member * rows : (member + 1) * rows, width:] = low
    lengths = len_ref[...]

    def masked(keys, start, unit):
        scores = score_tile(keys, split_ref[unit])
        key_at = lax.broadcasted_iota(jnp.int32, scores.shape, 0)
        return jnp.where(key_at < lengths - start, scores, NEG)

    def key_columns(unit):
        return pl.ds(pl.multiple_of(unit * width, width), width)

    def value_columns(unit):
        return pl.ds(pl.multiple_of((units + unit) * width, width), width)

    tops = [
        jnp.max(masked(first_ref[:, key_columns(unit)], 0, unit), axis=0, keepdims=True)
        for unit in range(units)
    ]

    def first(item):
        slot, unit = item
        return masked(pairs[slot][:, key_columns(unit)], starts[slot], unit)

    def second(item, scores):
        slot, unit = item
        powers = jnp.exp2(scores - tops[unit])
        sums = row_sums(powers)
        sum_ref[unit] = sums if slot == 0 else sum_ref[unit] + sums
        return powers.astype(jnp.bfloat16)

    def third(item, powers):
        slot, unit = item
        values = pairs[slot][:, value_columns(unit)].T
        added = jnp.dot(values, powers, preferred_element_type=jnp.float32)
        acc_ref[unit] = added if slot == 0 else acc_ref[unit] + added

    pipelined(
        [(slot, unit) for slot in range(slots) for unit in range(units)], first, second, third
    )

    @pl.when(jnp.max(sum_ref[...]) > BOUND)
    def _():
        def one(unit, carry):
            acc = jnp.zeros(acc_ref.shape[1:], jnp.float32)
            total = jnp.zeros(sum_ref.shape[1:], jnp.float32)
            top = jnp.full(lengths.shape, NEG, jnp.float32)
            for slot in range(slots):
                scores = masked(pairs[slot][:, key_columns(unit)], starts[slot], unit)
                raised = jnp.maximum(top, jnp.max(scores, axis=0, keepdims=True))
                powers = jnp.exp2(scores - raised)
                factor = jnp.exp2(top - raised)
                total = total * factor + row_sums(powers)
                acc = acc * factor + jnp.dot(
                    pairs[slot][:, value_columns(unit)].T,
                    powers.astype(jnp.bfloat16),
                    preferred_element_type=jnp.float32,
                )
                top = raised
            acc_ref[unit], sum_ref[unit] = acc, total
            return carry

        lax.fori_loop(0, units, one, 0)

    for unit in range(units):
        total = jnp.sum(sum_ref[unit], axis=0, keepdims=True)
        context = (acc_ref[unit] / total).T.astype(o_ref.dtype)
        for member in range(GROUP):
            head = unit * GROUP + member
            o_ref[:, head * width : (head + 1) * width] = context[
                member * rows : (member + 1) * rows
            ]


def decode_attention(queries, lanes, pairs):
    rows, columns = queries.shape
    units = columns // (GROUP * HEAD_WIDTH)
    block_rows, block_columns = pairs[0].shape
    blocks = len(pairs)
    scores = rows * blocks * block_rows * columns // HEAD_WIDTH
    vmem = pl.BlockSpec(memory_space=pltpu.VMEM)
    return pl.pallas_call(
        decode_kernel,
        out_shape=jax.ShapeDtypeStruct(queries.shape, queries.dtype),
        in_specs=[vmem] * (2 + blocks),
        out_specs=vmem,
        scratch_shapes=[
            pltpu.VMEM((block_rows, units * HEAD_WIDTH), jnp.bfloat16),
            pltpu.VMEM((units, rows * GROUP, 2 * HEAD_WIDTH), jnp.bfloat16),
            pltpu.VMEM((units, HEAD_WIDTH, rows * GROUP), jnp.float32),
            pltpu.VMEM((units, 8, rows * GROUP), jnp.float32),
        ],
        compiler_params=pltpu.CompilerParams(vmem_limit_bytes=20 * MIB),
        cost_estimate=pl.CostEstimate(
            flops=4 * scores * HEAD_WIDTH,
            bytes_accessed=2 * blocks * block_rows * block_columns,
            transcendentals=scores,
        ),
        name="decode",
    )(queries, lanes, *pairs)


def rotate(array, distance):
    count = lax.axis_size("ctx")
    return lax.ppermute(array, "ctx", [(i, (i + distance) % count) for i in range(count)])


def swap(array):
    return lax.ppermute(array, "grp", [(0, 1), (1, 0)])


def reduce_over_heads(piece):
    count = lax.axis_size("head")
    me = lax.axis_index("head")
    power_of_two = count & (count - 1) == 0
    terms = [piece(me)]
    for step in range(1, count):
        if power_of_two:
            target, pairs = me ^ step, [(i, i ^ step) for i in range(count)]
        else:
            target = (me + step) % count
            pairs = [(i, (i + step) % count) for i in range(count)]
        terms.append(lax.ppermute(piece(target), "head", pairs))
    return terms


def total_of(terms):
    return sum(term.astype(jnp.float32) for term in terms).astype(jnp.bfloat16)


def project(spread, out_weight):
    chips, rows, columns = spread.shape
    count = lax.axis_size("head")
    chip, core = lax.axis_index("ctx"), lax.axis_index("grp")

    def share(context):
        partial = jnp.dot(
            context.reshape(-1, columns), out_weight, preferred_element_type=jnp.float32
        )
        return partial.astype(jnp.bfloat16).reshape(chips, rows, -1)

    def in_order(mine, other):
        both = jnp.where(
            core == 0, jnp.stack([mine, other], axis=1), jnp.stack([other, mine], axis=1)
        )
        return both.reshape(-1, both.shape[-1])

    def one(partial, slot):
        return lax.dynamic_index_in_dim(partial, slot % chips, 0, keepdims=False)

    swapped = swap(spread)
    if chips == count:
        sums = []
        for context in (spread, swapped):
            partial = share(context)
            sums.append(reduce_over_heads(lambda j: one(partial, chip + chips - j)))
        mine, other = total_of(sums[0]), total_of(sums[1])
        return in_order(mine[None], other[None])

    def by_chip(partial):
        return jnp.stack([one(partial, chip + chips - c) for c in range(chips)])

    partial = in_order(by_chip(share(spread)), by_chip(share(swapped)))
    kept = partial.shape[0] // count
    return total_of(
        reduce_over_heads(lambda j: lax.dynamic_slice_in_dim(partial, j * kept, kept, 0))
    )


def local(
    prompt_queries,
    rotated_prompt_keys,
    prompt_value_rows,
    continuation_queries,
    prefix_len,
    out_weight,
):
    chips = lax.axis_size("ctx")
    chip, core = lax.axis_index("ctx"), lax.axis_index("grp")
    own = jnp.concatenate([rotated_prompt_keys, prompt_value_rows], axis=1)
    own_rows = continuation_queries.shape[0]
    my_index = chip * 2 + core
    lengths = lax.dynamic_slice_in_dim(prefix_len, my_index * own_rows, own_rows, 0)
    lanes = jnp.tile(lengths, GROUP)[None, :]

    ahead = chips // 2
    pairs = {0: (own, swap(own))}
    up, down = rotate(own, 1), rotate(own, -1)
    state = prompt_part(prompt_queries, pairs[0], 0, False, None)
    up, down, state, lanes = lax.optimization_barrier((up, down, state, lanes))
    for hop in range(1, ahead + 1):
        up_here, down_here = up, down
        if hop < ahead:
            up = rotate(up_here, 1)
        if hop + 1 < chips - ahead:
            down = rotate(down_here, -1)
        pairs[hop] = (up_here, swap(up_here))
        if hop < chips - ahead:
            pairs[chips - hop] = (down_here, swap(down_here))
        if hop < ahead:
            state = prompt_part(prompt_queries, pairs[hop], hop, False, state)
            up, down, state = lax.optimization_barrier((up, down, state))

    context = decode_attention(
        continuation_queries,
        lanes,
        [array for distance in range(chips) for array in pairs[distance]],
    )
    context, state = lax.optimization_barrier((context, state))
    spread = [context] + [rotate(context, distance) for distance in range(1, chips)]
    for distance in range(ahead + 1, chips):
        state = prompt_part(prompt_queries, pairs[distance], distance, False, state)
    prompt_context = prompt_part(prompt_queries, pairs[ahead], ahead, True, state)
    prompt_context, spread = lax.optimization_barrier((prompt_context, spread))
    return (prompt_context, project(jnp.stack(spread), out_weight))


def solution(mesh):
    in_specs = (
        P(("ctx", "grp"), "head"),
        P(("ctx", "grp"), "head"),
        P(("ctx", "grp"), "head"),
        P(("ctx", "grp"), "head"),
        P(),
        P("head", ("ctx", "grp")),
    )
    out_specs = (P(("ctx", "grp"), "head"), P("head", ("ctx", "grp")))
    return jax.shard_map(local, mesh=mesh, in_specs=in_specs, out_specs=out_specs, check_vma=False)
```

```python
import functools
import math

import jax
import jax.numpy as jnp
from jax import lax
from jax.experimental import pallas as pl
from jax.experimental.pallas import tpu as pltpu
from jax.sharding import PartitionSpec as P

QUERY_HEADS = 64
KEY_VALUE_HEADS = 8
HEAD_WIDTH = 128
GROUP = QUERY_HEADS // KEY_VALUE_HEADS
UNITS = GROUP // 2

NEG = -1e30
SCALE = HEAD_WIDTH ** -0.5 * math.log2(math.e)
BOUND = 2.0**64
MIB = 1024 * 1024


def split_scaled(rows):
    scaled = rows.astype(jnp.float32) * SCALE
    high = scaled.astype(jnp.bfloat16)
    low = (scaled - high.astype(jnp.float32)).astype(jnp.bfloat16)
    return high, low


def score_tile(keys, queries):
    return lax.dot_general(
        jnp.concatenate([keys, keys], axis=1),
        queries,
        (((1,), (1,)), ((), ())),
        preferred_element_type=jnp.float32,
    )


def row_sums(powers):
    return jnp.sum(powers.reshape(-1, 8, powers.shape[1]), axis=0)


def pipelined(items, first, second, third):
    ahead = first(items[0])
    behind = None
    for place, item in enumerate(items):
        following = first(items[place + 1]) if place + 1 < len(items) else None
        if behind is not None:
            third(items[place - 1], behind)
        behind = second(item, ahead)
        ahead = following
    third(items[-1], behind)


def fill_split(q_ref, split_ref):
    for unit in range(split_ref.shape[0]):
        columns = slice(unit * HEAD_WIDTH, (unit + 1) * HEAD_WIDTH)
        high, low = split_scaled(q_ref[:, columns])
        split_ref[unit, :, :HEAD_WIDTH] = high
        split_ref[unit, :, HEAD_WIDTH:] = low


def later_blocks(key_refs, value_refs, split_ref, old, new):
    acc_old, sum_old, max_old = old
    acc_new, sum_new, max_new = new
    units = split_ref.shape[0]
    values = [ref[...].T for ref in value_refs]
    max_new[...] = max_old[...]

    def score(item):
        block, unit = item
        return score_tile(key_refs[block][...], split_ref[unit])

    def power(item, scores):
        block, unit = item
        powers = jnp.exp2(scores - max_old[unit])
        earlier = (sum_old if block == 0 else sum_new)[unit]
        sum_new[unit] = earlier + row_sums(powers)
        return powers.astype(jnp.bfloat16)

    def weigh(item, powers):
        block, unit = item
        earlier = (acc_old if block == 0 else acc_new)[unit]
        acc_new[unit] = earlier + jnp.dot(
            values[block], powers, preferred_element_type=jnp.float32
        )

    pipelined(
        [(block, unit) for block in range(len(key_refs)) for unit in range(units)],
        score,
        power,
        weigh,
    )

    @pl.when(jnp.max(sum_new[...]) > BOUND)
    def _():
        def one(unit, carry):
            acc, total, top = acc_old[unit], sum_old[unit], max_old[unit]
            for key_ref, value in zip(key_refs, values):
                scores = score_tile(key_ref[...], split_ref[unit])
                raised = jnp.maximum(top, jnp.max(scores, axis=0, keepdims=True))
                powers = jnp.exp2(scores - raised)
                factor = jnp.exp2(top - raised)
                total = total * factor + row_sums(powers)
                acc = acc * factor + jnp.dot(
                    value, powers.astype(jnp.bfloat16), preferred_element_type=jnp.float32
                )
                top = raised
            acc_new[unit], sum_new[unit], max_new[unit] = acc, total, top
            return carry

        lax.fori_loop(0, units, one, 0)


def write_context(o_ref, acc_ref, sum_ref):
    for unit in range(acc_ref.shape[0]):
        total = jnp.sum(sum_ref[unit], axis=0, keepdims=True)
        o_ref[:, unit * HEAD_WIDTH : (unit + 1) * HEAD_WIDTH] = (
            (acc_ref[unit] / total).T.astype(o_ref.dtype)
        )


def begin_kernel(q_ref, k_ref, v_ref, ko_ref, vo_ref, *refs):
    new, split_ref, old = refs[:3], refs[3], refs[4:]
    acc_own, sum_own, max_own = old
    fill_split(q_ref, split_ref)
    values = v_ref[...].T

    def score(unit):
        scores = score_tile(k_ref[...], split_ref[unit])
        key_at = lax.broadcasted_iota(jnp.int32, scores.shape, 0)
        row_at = lax.broadcasted_iota(jnp.int32, scores.shape, 1)
        return jnp.where(key_at <= row_at, scores, NEG)

    def power(unit, scores):
        top = jnp.max(scores, axis=0, keepdims=True)
        powers = jnp.exp2(scores - top)
        max_own[unit] = top
        sum_own[unit] = row_sums(powers)
        return powers.astype(jnp.bfloat16)

    def weigh(unit, powers):
        acc_own[unit] = jnp.dot(values, powers, preferred_element_type=jnp.float32)

    pipelined(list(range(split_ref.shape[0])), score, power, weigh)
    applies = lax.axis_index("grp") > 0

    @pl.when(jnp.logical_not(applies))
    def _():
        for source, target in zip(old, new):
            target[...] = source[...]

    @pl.when(applies)
    def _():
        later_blocks([ko_ref], [vo_ref], split_ref, old, new)


def hop_kernel(hops, ends, q_ref, *refs):
    blocks, refs = refs[: 4 * len(hops)], refs[4 * len(hops) :]
    states, refs = [refs[:3]], refs[3:]
    if ends:
        o_ref, split_ref, held = refs[0], refs[1], refs[2:]
        pair = [held[:3], held[3:]]
        states += [pair[number % 2] for number in range(len(hops))]
    else:
        states.append(refs[:3])
        split_ref = refs[3]
    chip = lax.axis_index("ctx")
    some = chip >= min(hops)

    @pl.when(jnp.logical_not(some))
    def _():
        if ends:
            write_context(o_ref, *states[0][:2])
        else:
            for source, target in zip(states[0], states[1]):
                target[...] = source[...]

    @pl.when(some)
    def _():
        fill_split(q_ref, split_ref)
        for number, hop in enumerate(hops):
            k_ref, v_ref, ko_ref, vo_ref = blocks[4 * number : 4 * number + 4]
            old, new = states[number], states[number + 1]

            @pl.when(chip >= hop)
            def _():
                later_blocks([k_ref, ko_ref], [v_ref, vo_ref], split_ref, old, new)

            if hop > min(hops):

                @pl.when(chip < hop)
                def _():
                    for source, target in zip(old, new):
                        target[...] = source[...]

        if ends:
            write_context(o_ref, *states[-1][:2])


def prompt_part(queries, pairs, hops, ends, state):
    opens = hops == (0,)
    rows, columns = queries.shape
    heads = columns // HEAD_WIDTH
    heads_kv = pairs[hops[0]][0].shape[1] // (2 * HEAD_WIDTH)
    steps_each = GROUP // UNITS
    wide = pl.BlockSpec((rows, UNITS * HEAD_WIDTH), lambda h: (0, h))
    key_spec = pl.BlockSpec((rows, HEAD_WIDTH), lambda h: (0, h // steps_each))
    value_spec = pl.BlockSpec((rows, HEAD_WIDTH), lambda h: (0, heads_kv + h // steps_each))
    depths = (HEAD_WIDTH, 8, 1)
    state_specs = [pl.BlockSpec((UNITS, depth, rows), lambda h: (h, 0, 0)) for depth in depths]
    held = [pltpu.VMEM((UNITS, depth, rows), jnp.float32) for depth in depths]
    scratch = [pltpu.VMEM((UNITS, rows, 2 * HEAD_WIDTH), jnp.bfloat16)]
    if opens or ends:
        scratch += held * (1 if opens else 2)
    if ends:
        out_specs, out_shape = wide, jax.ShapeDtypeStruct(queries.shape, queries.dtype)
    else:
        out_specs = state_specs
        out_shape = [jax.ShapeDtypeStruct((heads, depth, rows), jnp.float32) for depth in depths]
    scores = 2 * len(hops) * rows * rows * heads
    return pl.pallas_call(
        begin_kernel if opens else functools.partial(hop_kernel, hops, ends),
        out_shape=out_shape,
        grid_spec=pl.GridSpec(
            grid=(heads // UNITS,),
            in_specs=[wide]
            + [key_spec, value_spec] * (2 * len(hops))
            + ([] if opens else state_specs),
            out_specs=out_specs,
            scratch_shapes=scratch,
        ),
        compiler_params=pltpu.CompilerParams(vmem_limit_bytes=20 * MIB),
        cost_estimate=pl.CostEstimate(
            flops=4 * scores * HEAD_WIDTH, bytes_accessed=8 * queries.size, transcendentals=scores
        ),
        name="prompt_%d" % hops[0],
    )(
        queries,
        *[array for hop in hops for block in pairs[hop] for array in (block, block)],
        *(state or ()),
    )


def decode_kernel(q_ref, len_ref, *refs):
    slots = len(refs) - 5
    pairs = refs[:slots]
    o_ref, first_ref, split_ref, acc_ref, sum_ref = refs[slots:]
    rows = q_ref.shape[0]
    units = split_ref.shape[0]
    block_rows = first_ref.shape[0]
    width = HEAD_WIDTH
    chip, core = lax.axis_index("ctx"), lax.axis_index("grp")
    starts = []
    for slot in range(slots):
        at = chip - slot // 2
        at = jnp.where(at < 0, at + slots // 2, at)
        block = 2 * at + (core if slot % 2 == 0 else 1 - core)
        starts.append(block * block_rows)

        @pl.when(block == 0)
        def _():
            first_ref[...] = pairs[slot][:, : units * width]

    for unit in range(units):
        for member in range(GROUP):
            head = unit * GROUP + member
            high, low = split_scaled(q_ref[:, head * width : (head + 1) * width])
            split_ref[unit, member * rows : (member + 1) * rows, :width] = high
            split_ref[unit, member * rows : (member + 1) * rows, width:] = low
    lengths = len_ref[...]

    def masked(keys, start, unit):
        scores = score_tile(keys, split_ref[unit])
        key_at = lax.broadcasted_iota(jnp.int32, scores.shape, 0)
        return jnp.where(key_at < lengths - start, scores, NEG)

    def key_columns(unit):
        return pl.ds(pl.multiple_of(unit * width, width), width)

    def value_columns(unit):
        return pl.ds(pl.multiple_of((units + unit) * width, width), width)

    tops = [
        jnp.max(masked(first_ref[:, key_columns(unit)], 0, unit), axis=0, keepdims=True)
        for unit in range(units)
    ]

    def first(item):
        slot, unit = item
        return masked(pairs[slot][:, key_columns(unit)], starts[slot], unit)

    def second(item, scores):
        slot, unit = item
        powers = jnp.exp2(scores - tops[unit])
        sums = row_sums(powers)
        sum_ref[unit] = sums if slot == 0 else sum_ref[unit] + sums
        return powers.astype(jnp.bfloat16)

    def third(item, powers):
        slot, unit = item
        values = pairs[slot][:, value_columns(unit)].T
        added = jnp.dot(values, powers, preferred_element_type=jnp.float32)
        acc_ref[unit] = added if slot == 0 else acc_ref[unit] + added

    pipelined(
        [(slot, unit) for slot in range(slots) for unit in range(units)], first, second, third
    )

    @pl.when(jnp.max(sum_ref[...]) > BOUND)
    def _():
        def one(unit, carry):
            acc = jnp.zeros(acc_ref.shape[1:], jnp.float32)
            total = jnp.zeros(sum_ref.shape[1:], jnp.float32)
            top = jnp.full(lengths.shape, NEG, jnp.float32)
            for slot in range(slots):
                scores = masked(pairs[slot][:, key_columns(unit)], starts[slot], unit)
                raised = jnp.maximum(top, jnp.max(scores, axis=0, keepdims=True))
                powers = jnp.exp2(scores - raised)
                factor = jnp.exp2(top - raised)
                total = total * factor + row_sums(powers)
                acc = acc * factor + jnp.dot(
                    pairs[slot][:, value_columns(unit)].T,
                    powers.astype(jnp.bfloat16),
                    preferred_element_type=jnp.float32,
                )
                top = raised
            acc_ref[unit], sum_ref[unit] = acc, total
            return carry

        lax.fori_loop(0, units, one, 0)

    for unit in range(units):
        total = jnp.sum(sum_ref[unit], axis=0, keepdims=True)
        context = (acc_ref[unit] / total).T.astype(o_ref.dtype)
        for member in range(GROUP):
            head = unit * GROUP + member
            o_ref[:, head * width : (head + 1) * width] = context[
                member * rows : (member + 1) * rows
            ]


def decode_attention(queries, lanes, pairs):
    rows, columns = queries.shape
    units = columns // (GROUP * HEAD_WIDTH)
    block_rows, block_columns = pairs[0].shape
    blocks = len(pairs)
    scores = rows * blocks * block_rows * columns // HEAD_WIDTH
    vmem = pl.BlockSpec(memory_space=pltpu.VMEM)
    return pl.pallas_call(
        decode_kernel,
        out_shape=jax.ShapeDtypeStruct(queries.shape, queries.dtype),
        in_specs=[vmem] * (2 + blocks),
        out_specs=vmem,
        scratch_shapes=[
            pltpu.VMEM((block_rows, units * HEAD_WIDTH), jnp.bfloat16),
            pltpu.VMEM((units, rows * GROUP, 2 * HEAD_WIDTH), jnp.bfloat16),
            pltpu.VMEM((units, HEAD_WIDTH, rows * GROUP), jnp.float32),
            pltpu.VMEM((units, 8, rows * GROUP), jnp.float32),
        ],
        compiler_params=pltpu.CompilerParams(vmem_limit_bytes=20 * MIB),
        cost_estimate=pl.CostEstimate(
            flops=4 * scores * HEAD_WIDTH,
            bytes_accessed=2 * blocks * block_rows * block_columns,
            transcendentals=scores,
        ),
        name="decode",
    )(queries, lanes, *pairs)


def rotate(array, distance):
    count = lax.axis_size("ctx")
    return lax.ppermute(array, "ctx", [(i, (i + distance) % count) for i in range(count)])


def swap(array):
    return lax.ppermute(array, "grp", [(0, 1), (1, 0)])


def reduce_over_heads(piece):
    count = lax.axis_size("head")
    me = lax.axis_index("head")
    power_of_two = count & (count - 1) == 0
    terms = [piece(me)]
    for step in range(1, count):
        if power_of_two:
            target, pairs = me ^ step, [(i, i ^ step) for i in range(count)]
        else:
            target = (me + step) % count
            pairs = [(i, (i + step) % count) for i in range(count)]
        terms.append(lax.ppermute(piece(target), "head", pairs))
    return terms


def total_of(terms):
    return sum(term.astype(jnp.float32) for term in terms).astype(jnp.bfloat16)


def project(spread, out_weight):
    chips, rows, columns = spread.shape
    count = lax.axis_size("head")
    chip, core = lax.axis_index("ctx"), lax.axis_index("grp")

    def share(context):
        partial = jnp.dot(
            context.reshape(-1, columns), out_weight, preferred_element_type=jnp.float32
        )
        return partial.astype(jnp.bfloat16).reshape(chips, rows, -1)

    def in_order(mine, other):
        both = jnp.where(
            core == 0, jnp.stack([mine, other], axis=1), jnp.stack([other, mine], axis=1)
        )
        return both.reshape(-1, both.shape[-1])

    def one(partial, slot):
        return lax.dynamic_index_in_dim(partial, slot % chips, 0, keepdims=False)

    swapped = swap(spread)
    if chips == count:
        sums = []
        for context in (spread, swapped):
            partial = share(context)
            sums.append(reduce_over_heads(lambda j: one(partial, chip + chips - j)))
        mine, other = total_of(sums[0]), total_of(sums[1])
        return in_order(mine[None], other[None])

    def by_chip(partial):
        return jnp.stack([one(partial, chip + chips - c) for c in range(chips)])

    partial = in_order(by_chip(share(spread)), by_chip(share(swapped)))
    kept = partial.shape[0] // count
    return total_of(
        reduce_over_heads(lambda j: lax.dynamic_slice_in_dim(partial, j * kept, kept, 0))
    )


def local(
    prompt_queries,
    rotated_prompt_keys,
    prompt_value_rows,
    continuation_queries,
    prefix_len,
    out_weight,
):
    chips = lax.axis_size("ctx")
    chip, core = lax.axis_index("ctx"), lax.axis_index("grp")
    own = jnp.concatenate([rotated_prompt_keys, prompt_value_rows], axis=1)
    own_rows = continuation_queries.shape[0]
    my_index = chip * 2 + core
    lengths = lax.dynamic_slice_in_dim(prefix_len, my_index * own_rows, own_rows, 0)
    lanes = jnp.tile(lengths, GROUP)[None, :]

    ahead = chips // 2
    pairs = {0: (own, swap(own))}
    up, down = rotate(own, 1), rotate(own, -1)
    state = prompt_part(prompt_queries, pairs, (0,), False, None)
    up, state, lanes = lax.optimization_barrier((up, state, lanes))
    for hop in range(1, ahead + 1):
        up_here = up
        if hop < ahead:
            up = rotate(up_here, 1)
        pairs[hop] = (up_here, swap(up_here))
        if hop < ahead:
            state = prompt_part(prompt_queries, pairs, (hop,), False, state)
        if hop < chips - ahead:
            down_here, state = lax.optimization_barrier((down, state))
            if hop + 1 < chips - ahead:
                down = rotate(down_here, -1)
            pairs[chips - hop] = (down_here, swap(down_here))
        up, state = lax.optimization_barrier((up, state))

    context = decode_attention(
        continuation_queries,
        lanes,
        [array for distance in range(chips) for array in pairs[distance]],
    )
    context, state = lax.optimization_barrier((context, state))
    spread = [context] + [rotate(context, distance) for distance in range(1, chips)]
    prompt_context = prompt_part(
        prompt_queries, pairs, (*range(ahead + 1, chips), ahead), True, state
    )
    prompt_context, spread = lax.optimization_barrier((prompt_context, spread))
    return (prompt_context, project(jnp.stack(spread), out_weight))


def solution(mesh):
    in_specs = (
        P(("ctx", "grp"), "head"),
        P(("ctx", "grp"), "head"),
        P(("ctx", "grp"), "head"),
        P(("ctx", "grp"), "head"),
        P(),
        P("head", ("ctx", "grp")),
    )
    out_specs = (P(("ctx", "grp"), "head"), P("head", ("ctx", "grp")))
    return jax.shard_map(local, mesh=mesh, in_specs=in_specs, out_specs=out_specs, check_vma=False)
```

```python
import functools
import math

import jax
import jax.numpy as jnp
from jax import lax
from jax.experimental import pallas as pl
from jax.experimental.pallas import tpu as pltpu
from jax.sharding import PartitionSpec as P


QUERY_HEADS = 64
KEY_VALUE_HEADS = 8
HEAD_WIDTH = 128
GROUP = QUERY_HEADS // KEY_VALUE_HEADS
UNITS = GROUP // 2

NEG = -1e30
SCALE = HEAD_WIDTH ** -0.5 * math.log2(math.e)
BOUND = 2.0**64
MIB = 1024 * 1024


def split_scaled(rows):
    scaled = rows.astype(jnp.float32) * SCALE
    high = scaled.astype(jnp.bfloat16)
    low = (scaled - high.astype(jnp.float32)).astype(jnp.bfloat16)
    return high, low


def score_tile(keys, queries):
    return lax.dot_general(
        jnp.concatenate([keys, keys], axis=1),
        queries,
        (((1,), (1,)), ((), ())),
        preferred_element_type=jnp.float32,
    )


def row_sums(powers):
    return jnp.sum(powers.reshape(-1, 8, powers.shape[1]), axis=0)


def pipelined(items, first, second, third):
    ahead = first(items[0])
    behind = None
    for place, item in enumerate(items):
        following = first(items[place + 1]) if place + 1 < len(items) else None
        if behind is not None:
            third(items[place - 1], behind)
        behind = second(item, ahead)
        ahead = following
    third(items[-1], behind)


def fill_split(q_ref, split_ref):
    for unit in range(split_ref.shape[0]):
        columns = slice(unit * HEAD_WIDTH, (unit + 1) * HEAD_WIDTH)
        high, low = split_scaled(q_ref[:, columns])
        split_ref[unit, :, :HEAD_WIDTH] = high
        split_ref[unit, :, HEAD_WIDTH:] = low


def later_blocks(key_refs, value_refs, split_ref, old, new):
    acc_old, sum_old, max_old = old
    acc_new, sum_new, max_new = new
    units = split_ref.shape[0]
    values = [ref[...].T for ref in value_refs]
    max_new[...] = max_old[...]

    def score(item):
        block, unit = item
        return score_tile(key_refs[block][...], split_ref[unit])

    def power(item, scores):
        block, unit = item
        powers = jnp.exp2(scores - max_old[unit])
        earlier = (sum_old if block == 0 else sum_new)[unit]
        sum_new[unit] = earlier + row_sums(powers)
        return powers.astype(jnp.bfloat16)

    def weigh(item, powers):
        block, unit = item
        earlier = (acc_old if block == 0 else acc_new)[unit]
        acc_new[unit] = earlier + jnp.dot(
            values[block], powers, preferred_element_type=jnp.float32
        )

    pipelined(
        [(block, unit) for block in range(len(key_refs)) for unit in range(units)],
        score,
        power,
        weigh,
    )

    @pl.when(jnp.max(sum_new[...]) > BOUND)
    def _():
        def one(unit, carry):
            acc, total, top = acc_old[unit], sum_old[unit], max_old[unit]
            for key_ref, value in zip(key_refs, values):
                scores = score_tile(key_ref[...], split_ref[unit])
                raised = jnp.maximum(top, jnp.max(scores, axis=0, keepdims=True))
                powers = jnp.exp2(scores - raised)
                factor = jnp.exp2(top - raised)
                total = total * factor + row_sums(powers)
                acc = acc * factor + jnp.dot(
                    value, powers.astype(jnp.bfloat16), preferred_element_type=jnp.float32
                )
                top = raised
            acc_new[unit], sum_new[unit], max_new[unit] = acc, total, top
            return carry

        lax.fori_loop(0, units, one, 0)


def write_context(o_ref, acc_ref, sum_ref):
    for unit in range(acc_ref.shape[0]):
        total = jnp.sum(sum_ref[unit], axis=0, keepdims=True)
        o_ref[:, unit * HEAD_WIDTH : (unit + 1) * HEAD_WIDTH] = (
            (acc_ref[unit] / total).T.astype(o_ref.dtype)
        )


def begin_kernel(q_ref, k_ref, v_ref, ko_ref, vo_ref, *refs):
    new, split_ref, old = refs[:3], refs[3], refs[4:]
    acc_own, sum_own, max_own = old
    fill_split(q_ref, split_ref)
    values = v_ref[...].T

    def score(unit):
        scores = score_tile(k_ref[...], split_ref[unit])
        key_at = lax.broadcasted_iota(jnp.int32, scores.shape, 0)
        row_at = lax.broadcasted_iota(jnp.int32, scores.shape, 1)
        return jnp.where(key_at <= row_at, scores, NEG)

    def power(unit, scores):
        top = jnp.max(scores, axis=0, keepdims=True)
        powers = jnp.exp2(scores - top)
        max_own[unit] = top
        sum_own[unit] = row_sums(powers)
        return powers.astype(jnp.bfloat16)

    def weigh(unit, powers):
        acc_own[unit] = jnp.dot(values, powers, preferred_element_type=jnp.float32)

    pipelined(list(range(split_ref.shape[0])), score, power, weigh)
    applies = lax.axis_index("grp") > 0

    @pl.when(jnp.logical_not(applies))
    def _():
        for source, target in zip(old, new):
            target[...] = source[...]

    @pl.when(applies)
    def _():
        later_blocks([ko_ref], [vo_ref], split_ref, old, new)


def hop_kernel(hops, ends, q_ref, *refs):
    blocks, refs = refs[: 4 * len(hops)], refs[4 * len(hops) :]
    states, refs = [refs[:3]], refs[3:]
    if ends:
        o_ref, split_ref, held = refs[0], refs[1], refs[2:]
        pair = [held[:3], held[3:]]
        states += [pair[number % 2] for number in range(len(hops))]
    else:
        states.append(refs[:3])
        split_ref = refs[3]
    chip = lax.axis_index("ctx")
    some = chip >= min(hops)

    @pl.when(jnp.logical_not(some))
    def _():
        if ends:
            write_context(o_ref, *states[0][:2])
        else:
            for source, target in zip(states[0], states[1]):
                target[...] = source[...]

    @pl.when(some)
    def _():
        fill_split(q_ref, split_ref)
        for number, hop in enumerate(hops):
            k_ref, v_ref, ko_ref, vo_ref = blocks[4 * number : 4 * number + 4]
            old, new = states[number], states[number + 1]

            @pl.when(chip >= hop)
            def _():
                later_blocks([k_ref, ko_ref], [v_ref, vo_ref], split_ref, old, new)

            if hop > min(hops):

                @pl.when(chip < hop)
                def _():
                    for source, target in zip(old, new):
                        target[...] = source[...]

        if ends:
            write_context(o_ref, *states[-1][:2])


def prompt_part(queries, pairs, hops, ends, state):
    opens = hops == (0,)
    rows, columns = queries.shape
    heads = columns // HEAD_WIDTH
    heads_kv = pairs[hops[0]][0].shape[1] // (2 * HEAD_WIDTH)
    steps_each = GROUP // UNITS
    wide = pl.BlockSpec((rows, UNITS * HEAD_WIDTH), lambda h: (0, h))
    key_spec = pl.BlockSpec((rows, HEAD_WIDTH), lambda h: (0, h // steps_each))
    value_spec = pl.BlockSpec((rows, HEAD_WIDTH), lambda h: (0, heads_kv + h // steps_each))
    depths = (HEAD_WIDTH, 8, 1)
    state_specs = [pl.BlockSpec((UNITS, depth, rows), lambda h: (h, 0, 0)) for depth in depths]
    held = [pltpu.VMEM((UNITS, depth, rows), jnp.float32) for depth in depths]
    scratch = [pltpu.VMEM((UNITS, rows, 2 * HEAD_WIDTH), jnp.bfloat16)]
    if opens or ends:
        scratch += held * (1 if opens else 2)
    if ends:
        out_specs, out_shape = wide, jax.ShapeDtypeStruct(queries.shape, queries.dtype)
    else:
        out_specs = state_specs
        out_shape = [jax.ShapeDtypeStruct((heads, depth, rows), jnp.float32) for depth in depths]
    scores = 2 * len(hops) * rows * rows * heads
    return pl.pallas_call(
        begin_kernel if opens else functools.partial(hop_kernel, hops, ends),
        out_shape=out_shape,
        grid_spec=pl.GridSpec(
            grid=(heads // UNITS,),
            in_specs=[wide]
            + [key_spec, value_spec] * (2 * len(hops))
            + ([] if opens else state_specs),
            out_specs=out_specs,
            scratch_shapes=scratch,
        ),
        compiler_params=pltpu.CompilerParams(vmem_limit_bytes=20 * MIB),
        cost_estimate=pl.CostEstimate(
            flops=4 * scores * HEAD_WIDTH, bytes_accessed=8 * queries.size, transcendentals=scores
        ),
    )(
        queries,
        *[array for hop in hops for block in pairs[hop] for array in (block, block)],
        *(state or ()),
    )


def decode_kernel(q_ref, len_ref, *refs):
    slots = len(refs) - 5
    pairs = refs[:slots]
    o_ref, first_ref, split_ref, acc_ref, sum_ref = refs[slots:]
    rows = q_ref.shape[0]
    units = split_ref.shape[0]
    block_rows = first_ref.shape[0]
    width = HEAD_WIDTH
    chip, core = lax.axis_index("ctx"), lax.axis_index("grp")
    starts = []
    for slot in range(slots):
        at = chip - slot // 2
        at = jnp.where(at < 0, at + slots // 2, at)
        block = 2 * at + (core if slot % 2 == 0 else 1 - core)
        starts.append(block * block_rows)

        @pl.when(block == 0)
        def _():
            first_ref[...] = pairs[slot][:, : units * width]

    for unit in range(units):
        for member in range(GROUP):
            head = unit * GROUP + member
            high, low = split_scaled(q_ref[:, head * width : (head + 1) * width])
            split_ref[unit, member * rows : (member + 1) * rows, :width] = high
            split_ref[unit, member * rows : (member + 1) * rows, width:] = low
    lengths = len_ref[...]

    def masked(keys, start, unit):
        scores = score_tile(keys, split_ref[unit])
        key_at = lax.broadcasted_iota(jnp.int32, scores.shape, 0)
        return jnp.where(key_at < lengths - start, scores, NEG)

    def key_columns(unit):
        return pl.ds(pl.multiple_of(unit * width, width), width)

    def value_columns(unit):
        return pl.ds(pl.multiple_of((units + unit) * width, width), width)

    tops = [
        jnp.max(masked(first_ref[:, key_columns(unit)], 0, unit), axis=0, keepdims=True)
        for unit in range(units)
    ]

    def first(item):
        slot, unit = item
        return masked(pairs[slot][:, key_columns(unit)], starts[slot], unit)

    def second(item, scores):
        slot, unit = item
        powers = jnp.exp2(scores - tops[unit])
        sums = row_sums(powers)
        sum_ref[unit] = sums if slot == 0 else sum_ref[unit] + sums
        return powers.astype(jnp.bfloat16)

    def third(item, powers):
        slot, unit = item
        values = pairs[slot][:, value_columns(unit)].T
        added = jnp.dot(values, powers, preferred_element_type=jnp.float32)
        acc_ref[unit] = added if slot == 0 else acc_ref[unit] + added

    pipelined(
        [(slot, unit) for slot in range(slots) for unit in range(units)], first, second, third
    )

    @pl.when(jnp.max(sum_ref[...]) > BOUND)
    def _():
        def one(unit, carry):
            acc = jnp.zeros(acc_ref.shape[1:], jnp.float32)
            total = jnp.zeros(sum_ref.shape[1:], jnp.float32)
            top = jnp.full(lengths.shape, NEG, jnp.float32)
            for slot in range(slots):
                scores = masked(pairs[slot][:, key_columns(unit)], starts[slot], unit)
                raised = jnp.maximum(top, jnp.max(scores, axis=0, keepdims=True))
                powers = jnp.exp2(scores - raised)
                factor = jnp.exp2(top - raised)
                total = total * factor + row_sums(powers)
                acc = acc * factor + jnp.dot(
                    pairs[slot][:, value_columns(unit)].T,
                    powers.astype(jnp.bfloat16),
                    preferred_element_type=jnp.float32,
                )
                top = raised
            acc_ref[unit], sum_ref[unit] = acc, total
            return carry

        lax.fori_loop(0, units, one, 0)

    for unit in range(units):
        total = jnp.sum(sum_ref[unit], axis=0, keepdims=True)
        context = (acc_ref[unit] / total).T.astype(o_ref.dtype)
        for member in range(GROUP):
            head = unit * GROUP + member
            o_ref[:, head * width : (head + 1) * width] = context[
                member * rows : (member + 1) * rows
            ]


def decode_attention(queries, lanes, pairs):
    rows, columns = queries.shape
    units = columns // (GROUP * HEAD_WIDTH)
    block_rows, block_columns = pairs[0].shape
    blocks = len(pairs)
    scores = rows * blocks * block_rows * columns // HEAD_WIDTH
    vmem = pl.BlockSpec(memory_space=pltpu.VMEM)
    return pl.pallas_call(
        decode_kernel,
        out_shape=jax.ShapeDtypeStruct(queries.shape, queries.dtype),
        in_specs=[vmem] * (2 + blocks),
        out_specs=vmem,
        scratch_shapes=[
            pltpu.VMEM((block_rows, units * HEAD_WIDTH), jnp.bfloat16),
            pltpu.VMEM((units, rows * GROUP, 2 * HEAD_WIDTH), jnp.bfloat16),
            pltpu.VMEM((units, HEAD_WIDTH, rows * GROUP), jnp.float32),
            pltpu.VMEM((units, 8, rows * GROUP), jnp.float32),
        ],
        compiler_params=pltpu.CompilerParams(vmem_limit_bytes=20 * MIB),
        cost_estimate=pl.CostEstimate(
            flops=4 * scores * HEAD_WIDTH,
            bytes_accessed=2 * blocks * block_rows * block_columns,
            transcendentals=scores,
        ),
        name="decode",
    )(queries, lanes, *pairs)


def rotate(array, distance):
    count = lax.axis_size("ctx")
    return lax.ppermute(array, "ctx", [(i, (i + distance) % count) for i in range(count)])


def swap(array):
    return lax.ppermute(array, "grp", [(0, 1), (1, 0)])


def reduce_over_heads(piece):
    count = lax.axis_size("head")
    me = lax.axis_index("head")
    power_of_two = count & (count - 1) == 0
    terms = [piece(me)]
    for step in range(1, count):
        if power_of_two:
            target, pairs = me ^ step, [(i, i ^ step) for i in range(count)]
        else:
            target = (me + step) % count
            pairs = [(i, (i + step) % count) for i in range(count)]
        terms.append(lax.ppermute(piece(target), "head", pairs))
    return terms


def total_of(terms):
    return sum(term.astype(jnp.float32) for term in terms).astype(jnp.bfloat16)


def product_kernel(a_ref, b_ref, o_ref):
    o_ref[...] = jnp.dot(a_ref[...], b_ref[...], preferred_element_type=jnp.float32).astype(
        o_ref.dtype
    )


def product(a, b):
    vmem = pl.BlockSpec(memory_space=pltpu.VMEM)
    return pl.pallas_call(
        product_kernel,
        out_shape=jax.ShapeDtypeStruct((a.shape[0], b.shape[1]), a.dtype),
        in_specs=[vmem, vmem],
        out_specs=vmem,
        compiler_params=pltpu.CompilerParams(vmem_limit_bytes=20 * MIB),
        cost_estimate=pl.CostEstimate(
            flops=2 * a.size * b.shape[1], bytes_accessed=2 * b.size, transcendentals=0
        ),
        name="product",
    )(a, b)


def project(spread, out_weight):
    chips, rows, columns = spread.shape
    count = lax.axis_size("head")
    chip, core = lax.axis_index("ctx"), lax.axis_index("grp")

    def share(context):
        return product(context.reshape(-1, columns), out_weight).reshape(chips, rows, -1)

    def in_order(mine, other):
        both = jnp.where(
            core == 0, jnp.stack([mine, other], axis=1), jnp.stack([other, mine], axis=1)
        )
        return both.reshape(-1, both.shape[-1])

    def one(partial, slot):
        return lax.dynamic_index_in_dim(partial, slot % chips, 0, keepdims=False)

    swapped = swap(spread)
    if chips == count:
        sums = []
        for context in (spread, swapped):
            partial = share(context)
            sums.append(reduce_over_heads(lambda j: one(partial, chip + chips - j)))
        mine, other = total_of(sums[0]), total_of(sums[1])
        return in_order(mine[None], other[None])

    def by_chip(partial):
        return jnp.stack([one(partial, chip + chips - c) for c in range(chips)])

    partial = in_order(by_chip(share(spread)), by_chip(share(swapped)))
    kept = partial.shape[0] // count
    return total_of(
        reduce_over_heads(lambda j: lax.dynamic_slice_in_dim(partial, j * kept, kept, 0))
    )


def local(
    prompt_queries,
    rotated_prompt_keys,
    prompt_value_rows,
    continuation_queries,
    prefix_len,
    out_weight,
):
    chips = lax.axis_size("ctx")
    chip, core = lax.axis_index("ctx"), lax.axis_index("grp")
    own = jnp.concatenate([rotated_prompt_keys, prompt_value_rows], axis=1)
    own_rows = continuation_queries.shape[0]
    my_index = chip * 2 + core
    lengths = lax.dynamic_slice_in_dim(prefix_len, my_index * own_rows, own_rows, 0)
    lanes = jnp.tile(lengths, GROUP)[None, :]

    ahead = chips // 2
    pairs = {0: (own, swap(own))}
    up = rotate(own, 1)
    down = rotate(own, -1)
    state = prompt_part(prompt_queries, pairs, (0,), False, None)
    up, state, lanes = lax.optimization_barrier((up, state, lanes))
    for hop in range(1, ahead + 1):
        up_here = up
        if hop < ahead:
            up = rotate(up_here, 1)
        pairs[hop] = (up_here, swap(up_here))
        if hop < ahead:
            state = prompt_part(prompt_queries, pairs, (hop,), False, state)
        if hop < chips - ahead:
            down_here, state = lax.optimization_barrier((down, state))
            if hop + 1 < chips - ahead:
                down = rotate(down_here, -1)
            pairs[chips - hop] = (down_here, swap(down_here))
        up, state = lax.optimization_barrier((up, state))

    context = decode_attention(
        continuation_queries,
        lanes,
        [array for distance in range(chips) for array in pairs[distance]],
    )
    context, state = lax.optimization_barrier((context, state))
    spread = [context] + [rotate(context, distance) for distance in range(1, chips)]
    prompt_context = prompt_part(
        prompt_queries, pairs, (*range(ahead + 1, chips), ahead), True, state
    )
    prompt_context, spread = lax.optimization_barrier((prompt_context, spread))
    return (prompt_context, project(jnp.stack(spread), out_weight))


def solution(mesh):
    in_specs = (
        P(("ctx", "grp"), "head"),
        P(("ctx", "grp"), "head"),
        P(("ctx", "grp"), "head"),
        P(("ctx", "grp"), "head"),
        P(),
        P("head", ("ctx", "grp")),
    )
    out_specs = (P(("ctx", "grp"), "head"), P("head", ("ctx", "grp")))

    return jax.shard_map(local, mesh=mesh, in_specs=in_specs, out_specs=out_specs, check_vma=False)
```
